32 devices in a mesh: head: 2 (over y), seq: 16 (over z, x, core).
Axes of the slice: x: 2, y: 2, z: 4, core: 2. Of those that a mesh axis runs over, the one named last changes fastest.
Arguments:
- queries: bfloat16 [2048, 4096], P(('seq', 'head')), may hold values from -20 to 20
- keys: bfloat16 [2048, 1024], P(('seq', 'head')), may hold values from -5 to 5
- values: bfloat16 [2048, 1024], P(('seq', 'head')), may hold values from -6 to 6
Outputs:
- attended: bfloat16 [2048, 4096], P(('seq', 'head'))
The draws below stay inside these ranges and needn't reach their ends.
All inputs are finite; a program needn't handle non-finite values.
Results may differ from the reference program's by a relative error of at most 0.0041.
Values may be sent and summed in bfloat16 or wider, within the bound.
A program may use at most 64 MiB of HBM per device.

```python
import math
import jax
import jax.numpy as jnp
from jax import lax

QHEADS = 32
KV_HEADS = 8
HEAD_DIM = 128
SEQ = 2048


def drawn_pair(key):
    width_q = QHEADS * HEAD_DIM
    width_k = KV_HEADS * HEAD_DIM
    key_q = jax.random.fold_in(key, 101)
    key_k = jax.random.fold_in(key, 102)
    q_draw = jnp.clip(jax.random.normal(key_q, (SEQ, width_q), jnp.float32), -5.0, 5.0)
    k_draw = jnp.clip(jax.random.normal(key_k, (SEQ, width_k), jnp.float32), -5.0, 5.0)
    return (q_draw, k_draw)


def draw_queries(key, part):
    return drawn_pair(key)[0].astype(jnp.bfloat16)


def draw_keys(key, part):
    return drawn_pair(key)[1].astype(jnp.bfloat16)


def block_scale(own_key, extent, shards, smallest, top_value):
    def one(dim, shards_of):
        draws = jax.random.uniform(jax.random.fold_in(jax.random.fold_in(own_key, 6), dim), (shards_of,), jnp.float32, smallest / len(shards), top_value / len(shards))
        return jnp.repeat(jnp.exp(draws), extent[dim] // shards_of).reshape((-1,) + (1,) * (len(extent) - dim - 1))

    factor_of = one(*shards[0])
    for cut in shards[1:]:
        factor_of = factor_of * one(*cut)
    return factor_of


def bell_draw(rng, dims, scale, reach, pieces=(), kind=jnp.bfloat16):
    factor_of = block_scale(rng, dims, pieces, -0.22, 0.18) if pieces else 1.0
    values = jax.random.normal(rng, dims, jnp.float32) * scale * factor_of
    return jnp.minimum(jnp.maximum(values, -reach), reach).astype(kind)


def setup_inputs(seed: int = 0) -> dict:
    arg_keys = jax.random.split(jax.random.key(seed), 4)
    queries = draw_queries(jax.random.fold_in(arg_keys[3], 71), 0)
    keys = draw_keys(jax.random.fold_in(arg_keys[3], 71), 0)
    values = bell_draw(arg_keys[2], (SEQ, KV_HEADS * HEAD_DIM), 1.0, 6.0, ((0, 32),))
    return dict(queries=queries, keys=keys, values=values)


def attend_block(query_rows, query_pos, key_all, value_all, key_pos):
    rows = query_rows.shape[0]
    group = QHEADS // KV_HEADS
    qf = query_rows.astype(jnp.float32).reshape(rows, KV_HEADS, group, HEAD_DIM)
    score = jnp.einsum('tkgd,pkd->tkgp', qf, key_all) / math.sqrt(HEAD_DIM)
    allowed = (key_pos[None, :] <= query_pos[:, None])[:, None, None, :]
    score = jnp.where(allowed, score, jnp.float32(-1e+30))
    largest = lax.optimization_barrier(jnp.max(score, axis=-1, keepdims=True))
    weight = jnp.where(allowed, jnp.exp(score - largest), jnp.float32(0.0))
    total = lax.optimization_barrier(jnp.sum(weight, axis=-1))
    rounded = lax.optimization_barrier(weight.astype(jnp.bfloat16)).astype(jnp.float32)
    summed = jnp.einsum('tkgp,pkd->tkgd', rounded, value_all)
    result = summed / total[..., None]
    return result.reshape(rows, QHEADS * HEAD_DIM).astype(jnp.bfloat16)

def reference(queries, keys, values):
    key_all = keys.astype(jnp.float32).reshape(SEQ, KV_HEADS, HEAD_DIM)
    value_all = values.astype(jnp.float32).reshape(SEQ, KV_HEADS, HEAD_DIM)
    segment = SEQ // 8
    block = math.gcd(segment, 128)
    outputs = []
    for part_index in range(8):
        limit = (part_index + 1) * segment
        key_pos = jnp.arange(limit, dtype=jnp.int32)
        rows = queries[part_index * segment:limit].reshape(segment // block, block, QHEADS * HEAD_DIM)
        positions = (part_index * segment + jnp.arange(segment, dtype=jnp.int32)).reshape(segment // block, block)

        def one_block(pair):
            return attend_block(pair[0], pair[1], key_all[:limit], value_all[:limit], key_pos)
        result = lax.map(one_block, (rows, positions))
        outputs.append(result.reshape(segment, QHEADS * HEAD_DIM))
    return jnp.concatenate(outputs, axis=0)
```

```python
import functools
import math

import jax
import jax.numpy as jnp
from jax import lax
from jax.experimental import pallas as pl
from jax.experimental.pallas import tpu as pltpu
from jax.sharding import PartitionSpec as P

HEAD_DIM = 128
TILE = 256
MESH = pl.DeviceIdType.MESH
NEG = -1e30


def kernel(
    cfg, q_in, k_in, v_in, out_ref, q_stage, kv_stage, q_all, kv_all, largest, summed, result,
    load_sem, own_sem, kv_send, kv_recv, q_send, q_recv, rise_send, up_send, up_recv, out_send, out_recv,
):
    heads, planes, inner, group, rows, chunk = cfg
    members = heads * inner
    plane_rows = members * rows
    chunks = plane_rows // chunk
    width = group * HEAD_DIM
    seq = lax.axis_index("seq")
    head = lax.axis_index("head")
    plane = seq // inner
    me = (seq % inner) * heads + head
    has_up = plane < planes - 1
    has_down = plane > 0

    def member(g):
        return {"head": g % heads, "seq": plane * inner + g // heads}

    def other_plane(step, g=me):
        return {"head": g % heads, "seq": (plane + step) * inner + g // heads}

    turns = inner % 2 == 0
    core = seq % 2 if turns else 0

    def flip(mask, start=me):
        g, bit = start, 1
        while bit < members:
            if mask & bit:
                g = g + bit * (1 - 2 * ((start // bit) % 2))
            bit *= 2
        return g

    def cols(g, size):
        return pl.ds(pl.multiple_of(g * size, HEAD_DIM), size)

    def block(g):
        return pl.ds(pl.multiple_of(g * rows, rows), rows)

    def position(g):
        return pl.ds(pl.multiple_of((plane * members + g) * rows, rows), rows)

    def piece(index):
        return pl.ds(pl.multiple_of(index * chunk, chunk), chunk)

    loads = [
        pltpu.make_async_copy(k_in, kv_stage.at[0], load_sem.at[0]),
        pltpu.make_async_copy(v_in, kv_stage.at[1], load_sem.at[1]),
        pltpu.make_async_copy(q_in, q_stage, load_sem.at[2]),
    ]
    own = [
        pltpu.make_async_copy(k_in.at[:, cols(me, HEAD_DIM)], kv_all.at[0, position(me)], own_sem.at[0]),
        pltpu.make_async_copy(v_in.at[:, cols(me, HEAD_DIM)], kv_all.at[1, position(me)], own_sem.at[1]),
        pltpu.make_async_copy(q_in.at[:, cols(me, width)], q_all.at[block(me)], own_sem.at[2]),
    ]
    for copy in loads + own:
        copy.start()

    barrier = pltpu.get_barrier_semaphore()
    for d in range(1, members):
        pl.semaphore_signal(
            barrier, inc=1, device_id=member((me + d) % members), device_id_type=MESH
        )

    @pl.when(has_up)
    def _():
        for g in range(members):
            pl.semaphore_signal(barrier, inc=1, device_id=other_plane(1, g), device_id_type=MESH)

    @pl.when(has_down)
    def _():
        for g in range(members):
            pl.semaphore_signal(barrier, inc=1, device_id=other_plane(-1, g), device_id_type=MESH)

    beside = jnp.minimum(plane, 1) + jnp.minimum(planes - 1 - plane, 1)
    pl.semaphore_wait(barrier, members - 1 + beside * members)

    def kv_copy(src, dst, to):
        return pltpu.make_async_remote_copy(
            src_ref=kv_stage.at[:, :, cols(dst, HEAD_DIM)],
            dst_ref=kv_all.at[:, position(src)],
            send_sem=kv_send.at[dst],
            recv_sem=kv_recv.at[src],
            device_id=member(to),
            device_id_type=MESH,
        )

    def q_copy(src, dst, to):
        return pltpu.make_async_remote_copy(
            src_ref=q_stage.at[:, cols(dst, width)],
            dst_ref=q_all.at[block(src)],
            send_sem=q_send.at[dst],
            recv_sem=q_recv.at[src],
            device_id=member(to),
            device_id_type=MESH,
        )

    def up_copy(index):
        return pltpu.make_async_remote_copy(
            src_ref=kv_all.at[:, piece(index)],
            dst_ref=kv_all.at[:, piece(index)],
            send_sem=up_send.at[index],
            recv_sem=up_recv.at[index],
            device_id=other_plane(1),
            device_id_type=MESH,
        )

    def rise_copy(dst):
        return pltpu.make_async_remote_copy(
            src_ref=kv_stage.at[:, :, cols(dst, HEAD_DIM)],
            dst_ref=kv_all.at[:, position(me)],
            send_sem=rise_send.at[dst],
            recv_sem=up_recv.at[plane * chunks + me // (members // chunks)],
            device_id=other_plane(1, dst),
            device_id_type=MESH,
        )

    def out_copy(src, dst, to):
        return pltpu.make_async_remote_copy(
            src_ref=result.at[block(dst)],
            dst_ref=out_ref.at[:, cols(src, width)],
            send_sem=out_send.at[dst],
            recv_sem=out_recv.at[src],
            device_id=member(to),
            device_id_type=MESH,
        )

    far_first = sorted(range(members), key=lambda m: (m < members // 2, m % 2, m))
    near_first = sorted(range(members), key=lambda m: (m * chunks // members, m % 2, m))
    if turns:
        sends = sorted(far_first, key=lambda m: (m // heads) % 2)
    else:
        sends = far_first
    peers = [flip(mask, me - core * heads) for mask in sends]

    def start_all(copy_of):
        for to in peers:

            @pl.when(to != me)
            def _(to=to):
                copy_of(me, to, to).start()

    loads[0].wait()
    loads[1].wait()
    start_all(kv_copy)

    @pl.when(has_up)
    def _():
        for to in peers:
            rise_copy(to).start()

    loads[2].wait()
    start_all(q_copy)

    for mask in near_first:
        src = flip(mask)
        if mask:
            kv_copy(src, me, src).wait_recv()
        else:
            own[0].wait()
            own[1].wait()

    def receive(index):
        up_copy(index).wait_recv()

        @pl.when(has_up)
        def _():
            up_copy(index).start()

    per_chunk = members // chunks

    def nearest(c):
        return (me // per_chunk + c) % chunks

    ahead = jnp.minimum(plane, 1)
    if turns:
        ahead = jnp.where(core == 0, plane, ahead)
    ahead = jnp.where(has_up, ahead, 0)

    def forward(step, carry):
        for c in range(chunks):
            receive((plane - step) * chunks + nearest(c))
        return carry

    lax.fori_loop(1, ahead + 1, forward, 0)

    own[2].wait()
    for mask in range(1, members):
        src = flip(mask)
        q_copy(src, me, src).wait_recv()

    scale = math.log2(math.e) / math.sqrt(HEAD_DIM)
    ones = jnp.ones((chunk, HEAD_DIM), jnp.bfloat16)

    def attend(index, tiles, first, masked):
        keys = kv_all[0, piece(index), :]
        values = jnp.concatenate([kv_all[1, piece(index), :], ones], axis=1)
        for r in tiles:
            for j in range(group):
                q = q_all[r * chunk:(r + 1) * chunk, j * HEAD_DIM:(j + 1) * HEAD_DIM]
                at = slice(j * plane_rows + r * chunk, j * plane_rows + (r + 1) * chunk)
                score = lax.dot_general(
                    q, keys, (((1,), (1,)), ((), ())), preferred_element_type=jnp.float32
                )
                if r == masked:
                    row = lax.broadcasted_iota(jnp.int32, score.shape, 0)
                    col = lax.broadcasted_iota(jnp.int32, score.shape, 1)
                    score = jnp.where(col <= row, score, NEG)
                top = jnp.broadcast_to(jnp.max(score, axis=1, keepdims=True), (chunk, HEAD_DIM))
                if not first:
                    before = largest[at, :]
                    top = jnp.maximum(before, top)
                spread = jnp.concatenate([top] * (chunk // HEAD_DIM), axis=1)
                weight = jnp.exp2((score - spread) * scale).astype(jnp.bfloat16)
                product = jnp.dot(weight, values, preferred_element_type=jnp.float32)
                if first:
                    summed[at, :] = product
                else:
                    shrink = jnp.exp2((before - top) * scale)
                    summed[at, :] = summed[at, :] * jnp.concatenate([shrink, shrink], axis=1) + product
                largest[at, :] = top

    for c in range(chunks):
        attend(plane * chunks + c, range(c, chunks), c == 0, c)

    def earlier(step, carry):
        for c in range(chunks):
            index = (plane - step) * chunks + nearest(c)

            @pl.when(step > ahead)
            def _():
                receive(index)

            attend(index, range(chunks), False, -1)
        return carry

    lax.fori_loop(1, plane + 1, earlier, 0)

    def finish(g):
        for j in range(group):
            at = pl.ds(pl.multiple_of(j * plane_rows + g * rows, rows), rows)
            result[block(g), j * HEAD_DIM:(j + 1) * HEAD_DIM] = (
                summed[at, :HEAD_DIM] / summed[at, HEAD_DIM:]
            ).astype(jnp.bfloat16)

    for mask in far_first:
        to = flip(mask)
        finish(to)
        if mask:
            out_copy(me, to, to).start()
    keep = pltpu.make_async_copy(result.at[block(me)], out_ref.at[:, cols(me, width)], own_sem.at[3])
    keep.start()

    for d in range(1, members):
        to = (me + d) % members
        kv_copy(me, to, to).wait_send()
        q_copy(me, to, to).wait_send()

    @pl.when(has_up)
    def _():
        def sent(index, carry):
            up_copy(index).wait_send()
            return carry

        lax.fori_loop(0, plane * chunks, sent, 0)
        for mask in range(members):
            rise_copy(mask).wait_send()

    for d in range(1, members):
        src = (me + d) % members
        out_copy(src, me, src).wait_recv()
        out_copy(me, src, src).wait_send()
    keep.wait()


def solution(mesh):
    heads, seqs = mesh.shape["head"], mesh.shape["seq"]

    def on_device(queries, keys, values):
        rows = queries.shape[0]
        members = keys.shape[1] // HEAD_DIM
        inner = members // heads
        planes = seqs // inner
        group = queries.shape[1] // keys.shape[1]
        plane_rows = members * rows
        chunk = math.gcd(plane_rows, TILE)
        total = planes * plane_rows
        pieces = total // chunk
        dma = pltpu.SemaphoreType.DMA
        cfg = (heads, planes, inner, group, rows, chunk)
        return pl.pallas_call(
            functools.partial(kernel, cfg),
            out_shape=pltpu.VMEM(queries.shape, jnp.bfloat16),
            in_specs=[pl.BlockSpec(memory_space=pl.ANY)] * 3,
            out_specs=pl.BlockSpec(memory_space=pltpu.VMEM),
            scratch_shapes=[
                pltpu.VMEM(queries.shape, jnp.bfloat16),
                pltpu.VMEM((2,) + keys.shape, jnp.bfloat16),
                pltpu.VMEM((plane_rows, group * HEAD_DIM), jnp.bfloat16),
                pltpu.VMEM((2, total, HEAD_DIM), jnp.bfloat16),
                pltpu.VMEM((group * plane_rows, HEAD_DIM), jnp.float32),
                pltpu.VMEM((group * plane_rows, 2 * HEAD_DIM), jnp.float32),
                pltpu.VMEM((plane_rows, group * HEAD_DIM), jnp.bfloat16),
                dma((3,)),
                dma((4,)),
                dma((members,)),
                dma((members,)),
                dma((members,)),
                dma((members,)),
                dma((members,)),
                dma((pieces,)),
                dma((pieces,)),
                dma((members,)),
                dma((members,)),
            ],
            compiler_params=pltpu.CompilerParams(collective_id=0, has_side_effects=True),
        )(queries, keys, values)

    spec = P(("seq", "head"), None)
    return jax.shard_map(
        on_device, mesh=mesh, in_specs=(spec, spec, spec), out_specs=spec, check_vma=False
    )
```

```python
import functools
import math

import jax
import jax.numpy as jnp
from jax import lax
from jax.experimental import pallas as pl
from jax.experimental.pallas import tpu as pltpu
from jax.sharding import PartitionSpec as P

HEAD_DIM = 128
TILE = 256
MESH = pl.DeviceIdType.MESH
NEG = -1e30


def kernel(
    cfg, q_in, k_in, v_in, out_ref, q_stage, kv_stage, q_all, kv_all, largest, summed, result,
    load_sem, own_sem, kv_send, kv_recv, q_send, q_recv, rise_send, up_send, up_recv, out_send, out_recv,
):
    heads, planes, inner, group, rows, chunk = cfg
    members = heads * inner
    plane_rows = members * rows
    chunks = plane_rows // chunk
    width = group * HEAD_DIM
    seq = lax.axis_index("seq")
    head = lax.axis_index("head")
    plane = seq // inner
    me = (seq % inner) * heads + head
    has_up = plane < planes - 1
    has_down = plane > 0

    def member(g):
        return {"head": g % heads, "seq": plane * inner + g // heads}

    def other_plane(step, g=me):
        return {"head": g % heads, "seq": (plane + step) * inner + g // heads}

    turns = inner % 2 == 0
    core = seq % 2 if turns else 0

    def flip(mask, start=me):
        g, bit = start, 1
        while bit < members:
            if mask & bit:
                g = g + bit * (1 - 2 * ((start // bit) % 2))
            bit *= 2
        return g

    def cols(g, size):
        return pl.ds(pl.multiple_of(g * size, HEAD_DIM), size)

    def block(g):
        return pl.ds(pl.multiple_of(g * rows, rows), rows)

    def position(g):
        return pl.ds(pl.multiple_of((plane * members + g) * rows, rows), rows)

    def piece(index):
        return pl.ds(pl.multiple_of(index * chunk, chunk), chunk)

    loads = [
        pltpu.make_async_copy(k_in, kv_stage.at[0], load_sem.at[0]),
        pltpu.make_async_copy(v_in, kv_stage.at[1], load_sem.at[1]),
        pltpu.make_async_copy(q_in, q_stage, load_sem.at[2]),
    ]
    own = [
        pltpu.make_async_copy(k_in.at[:, cols(me, HEAD_DIM)], kv_all.at[0, position(me)], own_sem.at[0]),
        pltpu.make_async_copy(v_in.at[:, cols(me, HEAD_DIM)], kv_all.at[1, position(me)], own_sem.at[1]),
        pltpu.make_async_copy(q_in.at[:, cols(me, width)], q_all.at[block(me)], own_sem.at[2]),
    ]
    for copy in loads + own:
        copy.start()

    barrier = pltpu.get_barrier_semaphore()
    for d in range(1, members):
        pl.semaphore_signal(
            barrier, inc=1, device_id=member((me + d) % members), device_id_type=MESH
        )

    @pl.when(has_up)
    def _():
        for g in range(members):
            pl.semaphore_signal(barrier, inc=1, device_id=other_plane(1, g), device_id_type=MESH)

    @pl.when(has_down)
    def _():
        for g in range(members):
            pl.semaphore_signal(barrier, inc=1, device_id=other_plane(-1, g), device_id_type=MESH)

    beside = jnp.minimum(plane, 1) + jnp.minimum(planes - 1 - plane, 1)
    pl.semaphore_wait(barrier, members - 1 + beside * members)

    def kv_copy(src, dst, to):
        return pltpu.make_async_remote_copy(
            src_ref=kv_stage.at[:, :, cols(dst, HEAD_DIM)],
            dst_ref=kv_all.at[:, position(src)],
            send_sem=kv_send.at[dst],
            recv_sem=kv_recv.at[src],
            device_id=member(to),
            device_id_type=MESH,
        )

    def q_copy(src, dst, to):
        return pltpu.make_async_remote_copy(
            src_ref=q_stage.at[:, cols(dst, width)],
            dst_ref=q_all.at[block(src)],
            send_sem=q_send.at[dst],
            recv_sem=q_recv.at[src],
            device_id=member(to),
            device_id_type=MESH,
        )

    def up_copy(index):
        return pltpu.make_async_remote_copy(
            src_ref=kv_all.at[:, piece(index)],
            dst_ref=kv_all.at[:, piece(index)],
            send_sem=up_send.at[index],
            recv_sem=up_recv.at[index],
            device_id=other_plane(1),
            device_id_type=MESH,
        )

    def rise_copy(dst):
        return pltpu.make_async_remote_copy(
            src_ref=kv_stage.at[:, :, cols(dst, HEAD_DIM)],
            dst_ref=kv_all.at[:, position(me)],
            send_sem=rise_send.at[dst],
            recv_sem=up_recv.at[plane * chunks + me // (members // chunks)],
            device_id=other_plane(1, dst),
            device_id_type=MESH,
        )

    def out_copy(src, dst, to):
        return pltpu.make_async_remote_copy(
            src_ref=result.at[block(dst)],
            dst_ref=out_ref.at[:, cols(src, width)],
            send_sem=out_send.at[dst],
            recv_sem=out_recv.at[src],
            device_id=member(to),
            device_id_type=MESH,
        )

    per_chunk = members // chunks
    near = me // per_chunk
    base = me - core * heads

    def peer(mask):
        return flip(mask, base)

    def reach(mask):
        g = mask // heads
        return (mask % heads > 0) + 2 * (g // (2 if turns else 1) > 0)

    core_of = {m: (m // heads) % 2 if turns else 0 for m in range(members)}
    far_first = sorted(range(members), key=lambda m: (core_of[m], -reach(m), m))
    near_first = sorted(range(members), key=lambda m: (core_of[m], reach(m), m))

    def start_all(copy_of, order):
        for to in map(peer, order):

            @pl.when(to != me)
            def _(to=to):
                copy_of(me, to, to).start()

    loads[0].wait()
    loads[1].wait()
    start_all(kv_copy, far_first)

    @pl.when(has_up)
    def _():
        for mask in far_first:
            rise_copy(peer(mask)).start()

    loads[2].wait()
    start_all(q_copy, near_first)

    def receive(index):
        up_copy(index).wait_recv()

        @pl.when(has_up)
        def _():
            up_copy(index).start()

    def nearest(c):
        return (near + c) % chunks

    def chunk_of(step, c):
        return (plane - step) * chunks + nearest(c)

    ahead = jnp.minimum(plane, 1)
    if turns:
        ahead = plane
    ahead = jnp.where(has_up, ahead, 0)

    def forward(step, carry):
        for c in range(chunks):
            receive(chunk_of(step, c))
        return carry

    scale = math.log2(math.e) / math.sqrt(HEAD_DIM)
    ones = jnp.ones((chunk, HEAD_DIM), jnp.bfloat16)

    def attend(index, tiles, first=False):
        keys = kv_all[0, piece(index), :]
        values = jnp.concatenate([kv_all[1, piece(index), :], ones], axis=1)
        for r in tiles:
            for j in range(group):
                q = q_all[piece(r), j * HEAD_DIM:(j + 1) * HEAD_DIM]
                at = pl.ds(pl.multiple_of(j * plane_rows + r * chunk, chunk), chunk)
                score = lax.dot_general(
                    q, keys, (((1,), (1,)), ((), ())), preferred_element_type=jnp.float32
                )
                if first:
                    row = lax.broadcasted_iota(jnp.int32, score.shape, 0)
                    col = lax.broadcasted_iota(jnp.int32, score.shape, 1)
                    score = jnp.where(col <= row, score, NEG)
                top = jnp.broadcast_to(jnp.max(score, axis=1, keepdims=True), (chunk, HEAD_DIM))
                if not first:
                    before = largest[at, :]
                    top = jnp.maximum(before, top)
                spread = jnp.concatenate([top] * (chunk // HEAD_DIM), axis=1)
                weight = jnp.exp2((score - spread) * scale).astype(jnp.bfloat16)
                product = jnp.dot(weight, values, preferred_element_type=jnp.float32)
                if first:
                    summed[at, :] = product
                else:
                    shrink = jnp.exp2((before - top) * scale)
                    summed[at, :] = summed[at, :] * jnp.concatenate([shrink, shrink], axis=1) + product
                largest[at, :] = top

    def kv_ready(mask):
        src = flip(mask)
        if mask:
            kv_copy(src, me, src).wait_recv()
        else:
            own[0].wait()
            own[1].wait()

    def q_ready(mask):
        src = flip(mask)
        if mask:
            q_copy(src, me, src).wait_recv()
        else:
            own[2].wait()

    def own_tile(shift):
        r = nearest(shift)
        attend(plane * chunks + r, [r], first=True)
        for c in range(chunks - 1):

            @pl.when(c < r)
            def _(c=c):
                attend(plane * chunks + c, [r])

    lax.fori_loop(1, ahead + 1, forward, 0)

    for mask in range(members):
        kv_ready(mask)
    for mask in range(per_chunk):
        q_ready(mask)
    own_tile(0)

    for mask in range(per_chunk, members):
        q_ready(mask)
    for shift in range(1, chunks):
        own_tile(shift)

    def earlier(step, count):
        for c in range(count):
            index = chunk_of(step, c)

            @pl.when(step > ahead)
            def _():
                receive(index)

            attend(index, range(chunks))

    def whole_step(step, carry):
        earlier(step, chunks)
        return carry

    lax.fori_loop(1, plane, whole_step, 0)

    final = chunk_of(plane, chunks - 1)

    @pl.when(has_down)
    def _():
        earlier(plane, chunks - 1)

        @pl.when(plane > ahead)
        def _():
            receive(final)

    def finish(g):
        for j in range(group):
            at = pl.ds(pl.multiple_of(j * plane_rows + g * rows, rows), rows)
            result[block(g), j * HEAD_DIM:(j + 1) * HEAD_DIM] = (
                summed[at, :HEAD_DIM] / summed[at, HEAD_DIM:]
            ).astype(jnp.bfloat16)

    for shift in reversed(range(chunks)):

        @pl.when(has_down)
        def _(shift=shift):
            attend(final, [nearest(shift)])

        tile = range(shift * per_chunk, (shift + 1) * per_chunk)
        for mask in sorted(tile, key=lambda m: (-reach(m), m)):
            to = flip(mask)
            finish(to)
            if mask:
                out_copy(me, to, to).start()
    keep = pltpu.make_async_copy(result.at[block(me)], out_ref.at[:, cols(me, width)], own_sem.at[3])
    keep.start()

    for d in range(1, members):
        to = (me + d) % members
        kv_copy(me, to, to).wait_send()
        q_copy(me, to, to).wait_send()

    @pl.when(has_up)
    def _():
        def sent(index, carry):
            up_copy(index).wait_send()
            return carry

        lax.fori_loop(0, plane * chunks, sent, 0)
        for mask in range(members):
            rise_copy(mask).wait_send()

    for d in range(1, members):
        src = (me + d) % members
        out_copy(src, me, src).wait_recv()
        out_copy(me, src, src).wait_send()
    keep.wait()


def solution(mesh):
    heads, seqs = mesh.shape["head"], mesh.shape["seq"]

    def on_device(queries, keys, values):
        rows = queries.shape[0]
        members = keys.shape[1] // HEAD_DIM
        inner = members // heads
        planes = seqs // inner
        group = queries.shape[1] // keys.shape[1]
        plane_rows = members * rows
        chunk = math.gcd(plane_rows, TILE)
        total = planes * plane_rows
        pieces = total // chunk
        dma = pltpu.SemaphoreType.DMA
        cfg = (heads, planes, inner, group, rows, chunk)
        return pl.pallas_call(
            functools.partial(kernel, cfg),
            out_shape=pltpu.VMEM(queries.shape, jnp.bfloat16),
            in_specs=[pl.BlockSpec(memory_space=pl.ANY)] * 3,
            out_specs=pl.BlockSpec(memory_space=pltpu.VMEM),
            scratch_shapes=[
                pltpu.VMEM(queries.shape, jnp.bfloat16),
                pltpu.VMEM((2,) + keys.shape, jnp.bfloat16),
                pltpu.VMEM((plane_rows, group * HEAD_DIM), jnp.bfloat16),
                pltpu.VMEM((2, total, HEAD_DIM), jnp.bfloat16),
                pltpu.VMEM((group * plane_rows, HEAD_DIM), jnp.float32),
                pltpu.VMEM((group * plane_rows, 2 * HEAD_DIM), jnp.float32),
                pltpu.VMEM((plane_rows, group * HEAD_DIM), jnp.bfloat16),
                dma((3,)),
                dma((4,)),
                dma((members,)),
                dma((members,)),
                dma((members,)),
                dma((members,)),
                dma((members,)),
                dma((pieces,)),
                dma((pieces,)),
                dma((members,)),
                dma((members,)),
            ],
            compiler_params=pltpu.CompilerParams(collective_id=0, has_side_effects=True),
        )(queries, keys, values)

    spec = P(("seq", "head"), None)
    return jax.shard_map(
        on_device, mesh=mesh, in_specs=(spec, spec, spec), out_specs=spec, check_vma=False
    )
```

```python
import functools
import math

import jax
import jax.numpy as jnp
from jax import lax
from jax.experimental import pallas as pl
from jax.experimental.pallas import tpu as pltpu
from jax.sharding import PartitionSpec as P

HEAD_DIM = 128
TILE = 256
MESH = pl.DeviceIdType.MESH
NEG = -1e30


def kernel(
    cfg, q_in, k_in, v_in, out_ref, q_stage, kv_stage, q_all, kv_all, largest, summed, result,
    load_sem, own_sem, go_sem, kv_send, kv_recv, q_send, q_recv, rise_send, up_send, up_recv, out_send, out_recv,
):
    heads, planes, inner, group, rows, chunk = cfg
    members = heads * inner
    plane_rows = members * rows
    chunks = plane_rows // chunk
    width = group * HEAD_DIM
    seq = lax.axis_index("seq")
    head = lax.axis_index("head")
    plane = seq // inner
    me = (seq % inner) * heads + head
    has_up = plane < planes - 1
    has_down = plane > 0

    def member(g):
        return {"head": g % heads, "seq": plane * inner + g // heads}

    def other_plane(step, g=me):
        return {"head": g % heads, "seq": (plane + step) * inner + g // heads}

    turns = inner % 2 == 0
    core = seq % 2 if turns else 0

    def flip(mask, start=me):
        g, bit = start, 1
        while bit < members:
            if mask & bit:
                g = g + bit * (1 - 2 * ((start // bit) % 2))
            bit *= 2
        return g

    def cols(g, size):
        return pl.ds(pl.multiple_of(g * size, HEAD_DIM), size)

    def block(g):
        return pl.ds(pl.multiple_of(g * rows, rows), rows)

    def position(g):
        return pl.ds(pl.multiple_of((plane * members + g) * rows, rows), rows)

    def piece(index):
        return pl.ds(pl.multiple_of(index * chunk, chunk), chunk)

    loads = [
        pltpu.make_async_copy(k_in, kv_stage.at[0], load_sem.at[0]),
        pltpu.make_async_copy(v_in, kv_stage.at[1], load_sem.at[1]),
        pltpu.make_async_copy(q_in, q_stage, load_sem.at[2]),
    ]
    own = [
        pltpu.make_async_copy(k_in.at[:, cols(me, HEAD_DIM)], kv_all.at[0, position(me)], own_sem.at[0]),
        pltpu.make_async_copy(v_in.at[:, cols(me, HEAD_DIM)], kv_all.at[1, position(me)], own_sem.at[1]),
        pltpu.make_async_copy(q_in.at[:, cols(me, width)], q_all.at[block(me)], own_sem.at[2]),
    ]
    for copy in loads + own:
        copy.start()

    barrier = pltpu.get_barrier_semaphore()
    for d in range(1, members):
        pl.semaphore_signal(
            barrier, inc=1, device_id=member((me + d) % members), device_id_type=MESH
        )

    @pl.when(has_down)
    def _():
        for g in range(members):
            pl.semaphore_signal(barrier, inc=1, device_id=other_plane(-1, g), device_id_type=MESH)

    above = jnp.minimum(planes - 1 - plane, 1)
    pl.semaphore_wait(barrier, members - 1 + above * members)

    def kv_copy(src, dst, to):
        return pltpu.make_async_remote_copy(
            src_ref=kv_stage.at[:, :, cols(dst, HEAD_DIM)],
            dst_ref=kv_all.at[:, position(src)],
            send_sem=kv_send.at[dst],
            recv_sem=kv_recv.at[src],
            device_id=member(to),
            device_id_type=MESH,
        )

    def q_copy(src, dst, to):
        return pltpu.make_async_remote_copy(
            src_ref=q_stage.at[:, cols(dst, width)],
            dst_ref=q_all.at[block(src)],
            send_sem=q_send.at[dst],
            recv_sem=q_recv.at[src],
            device_id=member(to),
            device_id_type=MESH,
        )

    def up_copy(index):
        return pltpu.make_async_remote_copy(
            src_ref=kv_all.at[:, piece(index)],
            dst_ref=kv_all.at[:, piece(index)],
            send_sem=up_send.at[index],
            recv_sem=up_recv.at[index],
            device_id=other_plane(1),
            device_id_type=MESH,
        )

    def rise_copy(dst):
        return pltpu.make_async_remote_copy(
            src_ref=kv_stage.at[:, :, cols(dst, HEAD_DIM)],
            dst_ref=kv_all.at[:, position(me)],
            send_sem=rise_send.at[dst],
            recv_sem=up_recv.at[plane * chunks + me // (members // chunks)],
            device_id=other_plane(1, dst),
            device_id_type=MESH,
        )

    def out_copy(src, dst, to):
        return pltpu.make_async_remote_copy(
            src_ref=result.at[block(dst)],
            dst_ref=out_ref.at[:, cols(src, width)],
            send_sem=out_send.at[dst],
            recv_sem=out_recv.at[src],
            device_id=member(to),
            device_id_type=MESH,
        )

    per_chunk = members // chunks
    near = me // per_chunk
    base = me - core * heads

    def peer(mask):
        return flip(mask, base)

    def reach(mask):
        g = mask // heads
        return (mask % heads > 0) + 2 * (g // (2 if turns else 1) > 0)

    core_of = {m: (m // heads) % 2 if turns else 0 for m in range(members)}
    far_first = sorted(range(members), key=lambda m: (core_of[m], -reach(m), m))
    near_first = sorted(range(members), key=lambda m: (core_of[m], reach(m), m))

    def start_all(copy_of, order):
        for to in map(peer, order):

            @pl.when(to != me)
            def _(to=to):
                copy_of(me, to, to).start()

    for load in loads:
        load.wait()

    for side in range(1 + max(core_of.values())):
        start_all(kv_copy, [m for m in far_first if core_of[m] == side])

        @pl.when(has_up)
        def _(side=side):
            for mask in far_first:
                if core_of[mask] == side:
                    rise_copy(peer(mask)).start()

        start_all(q_copy, [m for m in near_first if core_of[m] == side])

    def receive(index):
        up_copy(index).wait_recv()

        @pl.when(has_up)
        def _():
            up_copy(index).start()

    def nearest(c):
        return (near + c) % chunks

    def chunk_of(step, c):
        return (plane - step) * chunks + nearest(c)

    ahead = jnp.minimum(plane, 1)
    if turns:
        ahead = plane
    ahead = jnp.where(has_up, ahead, 0)

    waits = has_up & (plane > 1)

    def hold(at):
        if turns:

            @pl.when(waits & (core == 1) & at)
            def _():
                pl.semaphore_wait(go_sem, 1)

    def forward(step, carry):
        for c in range(chunks):
            if c == 1:
                hold(step == 1)
            receive(chunk_of(step, c))
        return carry

    scale = math.log2(math.e) / math.sqrt(HEAD_DIM)
    ones = jnp.ones((chunk, HEAD_DIM), jnp.bfloat16)

    def attend(index, tiles, first=False):
        keys = kv_all[0, piece(index), :]
        values = jnp.concatenate([kv_all[1, piece(index), :], ones], axis=1)
        for r in tiles:
            for j in range(group):
                q = q_all[piece(r), j * HEAD_DIM:(j + 1) * HEAD_DIM]
                at = pl.ds(pl.multiple_of(j * plane_rows + r * chunk, chunk), chunk)
                score = lax.dot_general(
                    q, keys, (((1,), (1,)), ((), ())), preferred_element_type=jnp.float32
                )
                if first:
                    row = lax.broadcasted_iota(jnp.int32, score.shape, 0)
                    col = lax.broadcasted_iota(jnp.int32, score.shape, 1)
                    score = jnp.where(col <= row, score, NEG)
                top = jnp.broadcast_to(jnp.max(score, axis=1, keepdims=True), (chunk, HEAD_DIM))
                if not first:
                    before = largest[at, :]
                    top = jnp.maximum(before, top)
                spread = jnp.concatenate([top] * (chunk // HEAD_DIM), axis=1)
                weight = jnp.exp2((score - spread) * scale).astype(jnp.bfloat16)
                product = jnp.dot(weight, values, preferred_element_type=jnp.float32)
                if first:
                    summed[at, :] = product
                else:
                    shrink = jnp.exp2((before - top) * scale)
                    summed[at, :] = summed[at, :] * jnp.concatenate([shrink, shrink], axis=1) + product
                largest[at, :] = top

    def kv_ready(mask):
        src = flip(mask)
        if mask:
            kv_copy(src, me, src).wait_recv()
        else:
            own[0].wait()
            own[1].wait()

    def q_ready(mask):
        src = flip(mask)
        if mask:
            q_copy(src, me, src).wait_recv()
        else:
            own[2].wait()

    def own_tile(shift):
        r = nearest(shift)
        attend(plane * chunks + r, [r], first=True)
        for c in range(chunks - 1):

            @pl.when(c < r)
            def _(c=c):
                attend(plane * chunks + c, [r])

    lax.fori_loop(1, ahead + 1, forward, 0)

    if turns:

        @pl.when(waits & (core == 0))
        def _():
            sibling = {"head": head, "seq": seq + 1}
            pl.semaphore_signal(go_sem, inc=1, device_id=sibling, device_id_type=MESH)

    for mask in range(members):
        kv_ready(mask)
    for mask in range(per_chunk):
        q_ready(mask)
    own_tile(0)

    for mask in range(per_chunk, members):
        q_ready(mask)
    for shift in range(1, chunks):
        own_tile(shift)

    def earlier(step, count):
        for c in range(count):
            index = chunk_of(step, c)

            @pl.when(step > ahead)
            def _():
                receive(index)

            attend(index, range(chunks))

    def whole_step(step, carry):
        earlier(step, chunks)
        return carry

    lax.fori_loop(1, plane, whole_step, 0)

    final = chunk_of(plane, chunks - 1)

    @pl.when(has_down)
    def _():
        earlier(plane, chunks - 1)

        @pl.when(plane > ahead)
        def _():
            receive(final)

    def finish(g):
        for j in range(group):
            at = pl.ds(pl.multiple_of(j * plane_rows + g * rows, rows), rows)
            result[block(g), j * HEAD_DIM:(j + 1) * HEAD_DIM] = (
                summed[at, :HEAD_DIM] / summed[at, HEAD_DIM:]
            ).astype(jnp.bfloat16)

    for shift in reversed(range(chunks)):

        @pl.when(has_down)
        def _(shift=shift):
            attend(final, [nearest(shift)])

        tile = range(shift * per_chunk, (shift + 1) * per_chunk)
        for mask in sorted(tile, key=lambda m: (-reach(m), m)):
            to = flip(mask)
            finish(to)
            if mask:
                out_copy(me, to, to).start()
    keep = pltpu.make_async_copy(result.at[block(me)], out_ref.at[:, cols(me, width)], own_sem.at[3])
    keep.start()

    for d in range(1, members):
        to = (me + d) % members
        kv_copy(me, to, to).wait_send()
        q_copy(me, to, to).wait_send()

    @pl.when(has_up)
    def _():
        def sent(index, carry):
            up_copy(index).wait_send()
            return carry

        lax.fori_loop(0, plane * chunks, sent, 0)
        for mask in range(members):
            rise_copy(mask).wait_send()

    for d in range(1, members):
        src = (me + d) % members
        out_copy(src, me, src).wait_recv()
        out_copy(me, src, src).wait_send()
    keep.wait()


def solution(mesh):
    heads, seqs = mesh.shape["head"], mesh.shape["seq"]

    def on_device(queries, keys, values):
        rows = queries.shape[0]
        members = keys.shape[1] // HEAD_DIM
        inner = members // heads
        planes = seqs // inner
        group = queries.shape[1] // keys.shape[1]
        plane_rows = members * rows
        chunk = math.gcd(plane_rows, TILE)
        total = planes * plane_rows
        pieces = total // chunk
        dma = pltpu.SemaphoreType.DMA
        cfg = (heads, planes, inner, group, rows, chunk)
        return pl.pallas_call(
            functools.partial(kernel, cfg),
            out_shape=pltpu.VMEM(queries.shape, jnp.bfloat16),
            in_specs=[pl.BlockSpec(memory_space=pl.ANY)] * 3,
            out_specs=pl.BlockSpec(memory_space=pltpu.VMEM),
            scratch_shapes=[
                pltpu.VMEM(queries.shape, jnp.bfloat16),
                pltpu.VMEM((2,) + keys.shape, jnp.bfloat16),
                pltpu.VMEM((plane_rows, group * HEAD_DIM), jnp.bfloat16),
                pltpu.VMEM((2, total, HEAD_DIM), jnp.bfloat16),
                pltpu.VMEM((group * plane_rows, HEAD_DIM), jnp.float32),
                pltpu.VMEM((group * plane_rows, 2 * HEAD_DIM), jnp.float32),
                pltpu.VMEM((plane_rows, group * HEAD_DIM), jnp.bfloat16),
                dma((3,)),
                dma((4,)),
                pltpu.SemaphoreType.REGULAR,
                dma((members,)),
                dma((members,)),
                dma((members,)),
                dma((members,)),
                dma((members,)),
                dma((pieces,)),
                dma((pieces,)),
                dma((members,)),
                dma((members,)),
            ],
            compiler_params=pltpu.CompilerParams(collective_id=0, has_side_effects=True),
        )(queries, keys, values)

    spec = P(("seq", "head"), None)
    return jax.shard_map(
        on_device, mesh=mesh, in_specs=(spec, spec, spec), out_specs=spec, check_vma=False
    )
```

```python
import functools
import math

import jax
import jax.numpy as jnp
from jax import lax
from jax.experimental import pallas as pl
from jax.experimental.pallas import tpu as pltpu
from jax.sharding import PartitionSpec as P

HEAD_DIM = 128
TILE = 256
MESH = pl.DeviceIdType.MESH
NEG = -1e30


def kernel(
    cfg, q_in, k_in, v_in, out_ref, q_stage, kv_stage, q_all, kv_all, largest, summed, result,
    load_sem, own_sem, go_sem, kv_send, kv_recv, q_send, q_recv, rise_send, up_send, up_recv, out_send, out_recv,
):
    heads, planes, inner, group, rows, chunk = cfg
    members = heads * inner
    plane_rows = members * rows
    chunks = plane_rows // chunk
    width = group * HEAD_DIM
    seq = lax.axis_index("seq")
    head = lax.axis_index("head")
    plane = seq // inner
    me = (seq % inner) * heads + head
    has_up = plane < planes - 1
    has_down = plane > 0

    def member(g):
        return {"head": g % heads, "seq": plane * inner + g // heads}

    def other_plane(step, g=me):
        return {"head": g % heads, "seq": (plane + step) * inner + g // heads}

    turns = inner % 2 == 0
    core = seq % 2 if turns else 0

    def flip(mask, start=me):
        g, bit = start, 1
        while bit < members:
            if mask & bit:
                g = g + bit * (1 - 2 * ((start // bit) % 2))
            bit *= 2
        return g

    def cols(g, size):
        return pl.ds(pl.multiple_of(g * size, HEAD_DIM), size)

    def block(g):
        return pl.ds(pl.multiple_of(g * rows, rows), rows)

    def position(g):
        return pl.ds(pl.multiple_of((plane * members + g) * rows, rows), rows)

    def piece(index):
        return pl.ds(pl.multiple_of(index * chunk, chunk), chunk)

    loads = [
        pltpu.make_async_copy(k_in, kv_stage.at[0], load_sem.at[0]),
        pltpu.make_async_copy(v_in, kv_stage.at[1], load_sem.at[1]),
        pltpu.make_async_copy(q_in, q_stage, load_sem.at[2]),
    ]
    own = [
        pltpu.make_async_copy(k_in.at[:, cols(me, HEAD_DIM)], kv_all.at[0, position(me)], own_sem.at[0]),
        pltpu.make_async_copy(v_in.at[:, cols(me, HEAD_DIM)], kv_all.at[1, position(me)], own_sem.at[1]),
        pltpu.make_async_copy(q_in.at[:, cols(me, width)], q_all.at[block(me)], own_sem.at[2]),
    ]
    for copy in loads + own:
        copy.start()

    barrier = pltpu.get_barrier_semaphore()
    for d in range(1, members):
        pl.semaphore_signal(
            barrier, inc=1, device_id=member((me + d) % members), device_id_type=MESH
        )

    @pl.when(has_down)
    def _():
        for g in range(members):
            pl.semaphore_signal(barrier, inc=1, device_id=other_plane(-1, g), device_id_type=MESH)

    above = jnp.minimum(planes - 1 - plane, 1)
    pl.semaphore_wait(barrier, members - 1 + above * members)

    def kv_copy(src, dst, to):
        return pltpu.make_async_remote_copy(
            src_ref=kv_stage.at[:, :, cols(dst, HEAD_DIM)],
            dst_ref=kv_all.at[:, position(src)],
            send_sem=kv_send.at[dst],
            recv_sem=kv_recv.at[src],
            device_id=member(to),
            device_id_type=MESH,
        )

    def q_copy(src, dst, to):
        return pltpu.make_async_remote_copy(
            src_ref=q_stage.at[:, cols(dst, width)],
            dst_ref=q_all.at[block(src)],
            send_sem=q_send.at[dst],
            recv_sem=q_recv.at[src],
            device_id=member(to),
            device_id_type=MESH,
        )

    def up_copy(index):
        return pltpu.make_async_remote_copy(
            src_ref=kv_all.at[:, piece(index)],
            dst_ref=kv_all.at[:, piece(index)],
            send_sem=up_send.at[index],
            recv_sem=up_recv.at[index],
            device_id=other_plane(1),
            device_id_type=MESH,
        )

    def rise_copy(dst):
        return pltpu.make_async_remote_copy(
            src_ref=kv_stage.at[:, :, cols(dst, HEAD_DIM)],
            dst_ref=kv_all.at[:, position(me)],
            send_sem=rise_send.at[dst],
            recv_sem=up_recv.at[plane * chunks + me // (members // chunks)],
            device_id=other_plane(1, dst),
            device_id_type=MESH,
        )

    def out_copy(src, dst, to):
        return pltpu.make_async_remote_copy(
            src_ref=result.at[block(dst)],
            dst_ref=out_ref.at[:, cols(src, width)],
            send_sem=out_send.at[dst],
            recv_sem=out_recv.at[src],
            device_id=member(to),
            device_id_type=MESH,
        )

    per_chunk = members // chunks
    near = me // per_chunk
    base = me - core * heads

    def peer(mask):
        return flip(mask, base)

    def reach(mask):
        g = mask // heads
        return (mask % heads > 0) + 2 * (g // (2 if turns else 1) > 0)

    core_of = {m: (m // heads) % 2 if turns else 0 for m in range(members)}
    far_first = sorted(range(members), key=lambda m: (core_of[m], -reach(m), m))
    near_first = sorted(range(members), key=lambda m: (core_of[m], reach(m), m))

    def start_all(copy_of, order):
        for to in map(peer, order):

            @pl.when(to != me)
            def _(to=to):
                copy_of(me, to, to).start()

    for load in loads:
        load.wait()

    for side in range(1 + max(core_of.values())):
        start_all(kv_copy, [m for m in far_first if core_of[m] == side])

        @pl.when(has_up)
        def _(side=side):
            for mask in far_first:
                if core_of[mask] == side:
                    rise_copy(peer(mask)).start()

        start_all(q_copy, [m for m in near_first if core_of[m] == side])

    def receive(index):
        up_copy(index).wait_recv()

        @pl.when(has_up)
        def _():
            up_copy(index).start()

    def nearest(c):
        return (near + c) % chunks

    def chunk_of(step, c):
        return (plane - step) * chunks + nearest(c)

    ahead = jnp.minimum(plane, 1)
    if turns:
        ahead = plane
    ahead = jnp.where(has_up, ahead, 0)

    def forward(step, carry):
        for c in range(chunks):
            receive(chunk_of(step, c))
        return carry

    relays = has_up & has_down
    leads = relays & (core == 0) & turns
    trails = relays & (core == 1) & turns

    def lead_sent(first, last):
        for c in range(first, last):
            up_copy(chunk_of(plane, c)).wait_send()

    def pass_turn():
        sibling = {"head": head, "seq": seq + 1}
        pl.semaphore_signal(go_sem, inc=1, device_id=sibling, device_id_type=MESH)

    def take_turn():
        pl.semaphore_wait(go_sem, 1)

    scale = math.log2(math.e) / math.sqrt(HEAD_DIM)
    ones = jnp.ones((chunk, HEAD_DIM), jnp.bfloat16)

    def attend(index, tiles, first=False):
        keys = kv_all[0, piece(index), :]
        values = jnp.concatenate([kv_all[1, piece(index), :], ones], axis=1)
        for r in tiles:
            for j in range(group):
                q = q_all[piece(r), j * HEAD_DIM:(j + 1) * HEAD_DIM]
                at = pl.ds(pl.multiple_of(j * plane_rows + r * chunk, chunk), chunk)
                score = lax.dot_general(
                    q, keys, (((1,), (1,)), ((), ())), preferred_element_type=jnp.float32
                )
                if first:
                    row = lax.broadcasted_iota(jnp.int32, score.shape, 0)
                    col = lax.broadcasted_iota(jnp.int32, score.shape, 1)
                    score = jnp.where(col <= row, score, NEG)
                top = jnp.broadcast_to(jnp.max(score, axis=1, keepdims=True), (chunk, HEAD_DIM))
                if not first:
                    before = largest[at, :]
                    top = jnp.maximum(before, top)
                spread = jnp.concatenate([top] * (chunk // HEAD_DIM), axis=1)
                weight = jnp.exp2((score - spread) * scale).astype(jnp.bfloat16)
                product = jnp.dot(weight, values, preferred_element_type=jnp.float32)
                if first:
                    summed[at, :] = product
                else:
                    shrink = jnp.exp2((before - top) * scale)
                    summed[at, :] = summed[at, :] * jnp.concatenate([shrink, shrink], axis=1) + product
                largest[at, :] = top

    def kv_ready(mask):
        src = flip(mask)
        if mask:
            kv_copy(src, me, src).wait_recv()
        else:
            own[0].wait()
            own[1].wait()

    def q_ready(mask):
        src = flip(mask)
        if mask:
            q_copy(src, me, src).wait_recv()
        else:
            own[2].wait()

    def own_tile(shift):
        r = nearest(shift)
        attend(plane * chunks + r, [r], first=True)
        for c in range(chunks - 1):

            @pl.when(c < r)
            def _(c=c):
                attend(plane * chunks + c, [r])

    if turns:

        @pl.when(leads)
        def _():
            lax.fori_loop(1, plane + 1, forward, 0)

            @pl.when(plane == 1)
            def _():
                lead_sent(0, chunks)
                pass_turn()

        @pl.when(trails)
        def _():
            @pl.when(plane == 1)
            def _():
                take_turn()
                forward(1, 0)

            @pl.when(plane > 1)
            def _():
                receive(chunk_of(1, 0))

    else:
        lax.fori_loop(1, ahead + 1, forward, 0)

    for mask in range(members):
        kv_ready(mask)
    for mask in range(per_chunk):
        q_ready(mask)
    own_tile(0)

    if turns:

        @pl.when(trails & (plane > 1))
        def _():
            take_turn()
            for c in range(1, chunks):
                receive(chunk_of(1, c))
            lax.fori_loop(2, plane, forward, 0)
            for c in range(chunks - 1):
                receive(chunk_of(plane, c))

    for mask in range(per_chunk, members):
        q_ready(mask)
    for shift in range(1, chunks):
        own_tile(shift)

    if turns:

        @pl.when(leads & (plane > 1))
        def _():
            lead_sent(0, 1)
            pass_turn()

        @pl.when(trails & (plane > 1))
        def _():
            receive(chunk_of(plane, chunks - 1))

    def earlier(step, count):
        for c in range(count):
            index = chunk_of(step, c)

            @pl.when(step > ahead)
            def _():
                receive(index)

            attend(index, range(chunks))

    def whole_step(step, carry):
        earlier(step, chunks)
        return carry

    lax.fori_loop(1, plane, whole_step, 0)

    final = chunk_of(plane, chunks - 1)

    @pl.when(has_down)
    def _():
        earlier(plane, chunks - 1)

        @pl.when(plane > ahead)
        def _():
            receive(final)

    def finish(g):
        for j in range(group):
            at = pl.ds(pl.multiple_of(j * plane_rows + g * rows, rows), rows)
            result[block(g), j * HEAD_DIM:(j + 1) * HEAD_DIM] = (
                summed[at, :HEAD_DIM] / summed[at, HEAD_DIM:]
            ).astype(jnp.bfloat16)

    for shift in reversed(range(chunks)):

        @pl.when(has_down)
        def _(shift=shift):
            attend(final, [nearest(shift)])

        tile = range(shift * per_chunk, (shift + 1) * per_chunk)
        for mask in sorted(tile, key=lambda m: (-reach(m), m)):
            to = flip(mask)
            finish(to)
            if mask:
                out_copy(me, to, to).start()
    keep = pltpu.make_async_copy(result.at[block(me)], out_ref.at[:, cols(me, width)], own_sem.at[3])
    keep.start()

    for d in range(1, members):
        to = (me + d) % members
        kv_copy(me, to, to).wait_send()
        q_copy(me, to, to).wait_send()

    @pl.when(has_up)
    def _():
        def sent(index, carry):
            @pl.when((index != chunk_of(plane, 0)) | jnp.logical_not(leads & (plane > 1)))
            def _():
                up_copy(index).wait_send()

            return carry

        done = jnp.where(leads & (plane == 1), chunks, 0) if turns else 0
        lax.fori_loop(done, plane * chunks, sent, 0)
        for mask in range(members):
            rise_copy(mask).wait_send()

    for d in range(1, members):
        src = (me + d) % members
        out_copy(src, me, src).wait_recv()
        out_copy(me, src, src).wait_send()
    keep.wait()


def solution(mesh):
    heads, seqs = mesh.shape["head"], mesh.shape["seq"]

    def on_device(queries, keys, values):
        rows = queries.shape[0]
        members = keys.shape[1] // HEAD_DIM
        inner = members // heads
        planes = seqs // inner
        group = queries.shape[1] // keys.shape[1]
        plane_rows = members * rows
        chunk = math.gcd(plane_rows, TILE)
        total = planes * plane_rows
        pieces = total // chunk
        dma = pltpu.SemaphoreType.DMA
        cfg = (heads, planes, inner, group, rows, chunk)
        return pl.pallas_call(
            functools.partial(kernel, cfg),
            out_shape=pltpu.VMEM(queries.shape, jnp.bfloat16),
            in_specs=[pl.BlockSpec(memory_space=pl.ANY)] * 3,
            out_specs=pl.BlockSpec(memory_space=pltpu.VMEM),
            scratch_shapes=[
                pltpu.VMEM(queries.shape, jnp.bfloat16),
                pltpu.VMEM((2,) + keys.shape, jnp.bfloat16),
                pltpu.VMEM((plane_rows, group * HEAD_DIM), jnp.bfloat16),
                pltpu.VMEM((2, total, HEAD_DIM), jnp.bfloat16),
                pltpu.VMEM((group * plane_rows, HEAD_DIM), jnp.float32),
                pltpu.VMEM((group * plane_rows, 2 * HEAD_DIM), jnp.float32),
                pltpu.VMEM((plane_rows, group * HEAD_DIM), jnp.bfloat16),
                dma((3,)),
                dma((4,)),
                pltpu.SemaphoreType.REGULAR,
                dma((members,)),
                dma((members,)),
                dma((members,)),
                dma((members,)),
                dma((members,)),
                dma((pieces,)),
                dma((pieces,)),
                dma((members,)),
                dma((members,)),
            ],
            compiler_params=pltpu.CompilerParams(collective_id=0, has_side_effects=True),
        )(queries, keys, values)

    spec = P(("seq", "head"), None)
    return jax.shard_map(
        on_device, mesh=mesh, in_specs=(spec, spec, spec), out_specs=spec, check_vma=False
    )
```

```python
import functools
import math

import jax
import jax.numpy as jnp
from jax import lax
from jax.experimental import pallas as pl
from jax.experimental.pallas import tpu as pltpu
from jax.sharding import PartitionSpec as P

HEAD_DIM = 128
TILE = 256
MESH = pl.DeviceIdType.MESH
NEG = -1e30


def kernel(
    cfg, q_in, k_in, v_in, out_ref, q_stage, kv_stage, q_all, kv_all, largest, summed, result,
    load_sem, go_sem, kv_send, kv_recv, q_send, q_recv, rise_send, up_send, up_recv, out_send, out_recv,
):
    heads, planes, inner, group, rows, chunk = cfg
    members = heads * inner
    plane_rows = members * rows
    chunks = plane_rows // chunk
    per_chunk = members // chunks
    width = group * HEAD_DIM
    seq = lax.axis_index("seq")
    head = lax.axis_index("head")
    plane = seq // inner
    me = (seq % inner) * heads + head
    near = me // per_chunk
    has_up = plane < planes - 1
    has_down = plane > 0

    def member(g):
        return {"head": g % heads, "seq": plane * inner + g // heads}

    def other_plane(step, g=me):
        return {"head": g % heads, "seq": (plane + step) * inner + g // heads}

    turns = inner % 2 == 0
    core = seq % 2 if turns else 0

    def flip(mask, start=me):
        g, bit = start, 1
        while bit < members:
            if mask & bit:
                g = g + bit * (1 - 2 * ((start // bit) % 2))
            bit *= 2
        return g

    def cols(g, size):
        return pl.ds(pl.multiple_of(g * size, HEAD_DIM), size)

    def block(g):
        return pl.ds(pl.multiple_of(g * rows, rows), rows)

    def position(g):
        return pl.ds(pl.multiple_of((plane * members + g) * rows, rows), rows)

    def plane_of(index):
        return pl.ds(pl.multiple_of(index * plane_rows, plane_rows), plane_rows)

    def piece(index):
        return pl.ds(pl.multiple_of(index * chunk, chunk), chunk)

    loads = [
        pltpu.make_async_copy(k_in, kv_stage.at[0], load_sem.at[0]),
        pltpu.make_async_copy(v_in, kv_stage.at[1], load_sem.at[0]),
        pltpu.make_async_copy(q_in, q_stage, load_sem.at[1]),
    ]
    own = [
        pltpu.make_async_copy(k_in.at[:, cols(me, HEAD_DIM)], kv_all.at[0, position(me)], kv_recv),
        pltpu.make_async_copy(v_in.at[:, cols(me, HEAD_DIM)], kv_all.at[1, position(me)], kv_recv),
        pltpu.make_async_copy(q_in.at[:, cols(me, width)], q_all.at[block(me)], q_recv.at[near]),
    ]
    for copy in loads + own:
        copy.start()

    barrier = pltpu.get_barrier_semaphore()
    for d in range(1, members):
        pl.semaphore_signal(
            barrier, inc=1, device_id=member((me + d) % members), device_id_type=MESH
        )

    @pl.when(has_down)
    def _():
        for g in range(members):
            pl.semaphore_signal(barrier, inc=1, device_id=other_plane(-1, g), device_id_type=MESH)

    above = jnp.minimum(planes - 1 - plane, 1)
    pl.semaphore_wait(barrier, members - 1 + above * members)

    def kv_copy(src, dst, to):
        return pltpu.make_async_remote_copy(
            src_ref=kv_stage.at[:, :, cols(dst, HEAD_DIM)],
            dst_ref=kv_all.at[:, position(src)],
            send_sem=kv_send,
            recv_sem=kv_recv,
            device_id=member(to),
            device_id_type=MESH,
        )

    def q_copy(src, dst, to):
        return pltpu.make_async_remote_copy(
            src_ref=q_stage.at[:, cols(dst, width)],
            dst_ref=q_all.at[block(src)],
            send_sem=q_send,
            recv_sem=q_recv.at[src // per_chunk],
            device_id=member(to),
            device_id_type=MESH,
        )

    def up_copy(index):
        return pltpu.make_async_remote_copy(
            src_ref=kv_all.at[:, piece(index)],
            dst_ref=kv_all.at[:, piece(index)],
            send_sem=up_send.at[index],
            recv_sem=up_recv.at[index],
            device_id=other_plane(1),
            device_id_type=MESH,
        )

    def rise_copy(dst):
        return pltpu.make_async_remote_copy(
            src_ref=kv_stage.at[:, :, cols(dst, HEAD_DIM)],
            dst_ref=kv_all.at[:, position(me)],
            send_sem=rise_send,
            recv_sem=up_recv.at[plane * chunks + near],
            device_id=other_plane(1, dst),
            device_id_type=MESH,
        )

    def out_copy(src, dst, to):
        return pltpu.make_async_remote_copy(
            src_ref=result.at[block(dst)],
            dst_ref=out_ref.at[:, cols(src, width)],
            send_sem=out_send,
            recv_sem=out_recv,
            device_id=member(to),
            device_id_type=MESH,
        )

    base = me - core * heads

    def peer(mask):
        return flip(mask, base)

    def reach(mask):
        g = mask // heads
        return (mask % heads > 0) + 2 * (g // (2 if turns else 1) > 0)

    core_of = {m: (m // heads) % 2 if turns else 0 for m in range(members)}
    far_first = sorted(range(members), key=lambda m: (core_of[m], -reach(m), m))
    near_first = sorted(range(members), key=lambda m: (core_of[m], reach(m), m))

    def start_all(copy_of, order):
        for to in map(peer, order):

            @pl.when(to != me)
            def _(to=to):
                copy_of(me, to, to).start()

    def wait_all(ref, sem):
        pltpu.make_async_copy(ref, ref, sem).wait()

    wait_all(kv_stage, load_sem.at[0])
    wait_all(q_stage, load_sem.at[1])

    for side in range(1 + max(core_of.values())):
        start_all(kv_copy, [m for m in far_first if core_of[m] == side])

        @pl.when(has_up)
        def _(side=side):
            for mask in far_first:
                if core_of[mask] == side:
                    rise_copy(peer(mask)).start()

        start_all(q_copy, [m for m in near_first if core_of[m] == side])

    def receive(index):
        wait_all(kv_all.at[:, piece(index)], up_recv.at[index])

        @pl.when(has_up)
        def _():
            up_copy(index).start()

    def nearest(c):
        return (near + c) % chunks

    def chunk_of(step, c):
        return (plane - step) * chunks + nearest(c)

    ahead = jnp.minimum(plane, 1)
    if turns:
        ahead = plane
    ahead = jnp.where(has_up, ahead, 0)

    def forward(step, carry):
        for c in range(chunks):
            receive(chunk_of(step, c))
        return carry

    relays = has_up & has_down
    leads = relays & (core == 0) & turns
    trails = relays & (core == 1) & turns

    def lead_sent(first, last):
        for c in range(first, last):
            up_copy(chunk_of(plane, c)).wait_send()

    def pass_turn():
        sibling = {"head": head, "seq": seq + 1}
        pl.semaphore_signal(go_sem, inc=1, device_id=sibling, device_id_type=MESH)

    def take_turn():
        pl.semaphore_wait(go_sem, 1)

    scale = math.log2(math.e) / math.sqrt(HEAD_DIM)
    sub = chunk // 2 if chunk >= 2 * HEAD_DIM else chunk
    per_sub = sub // rows

    def attend(at_keys, row0, size, first=False):
        keys = kv_all[0, at_keys, :]
        count = keys.shape[0]
        ones = jnp.ones((count, HEAD_DIM), jnp.bfloat16)
        values = jnp.concatenate([kv_all[1, at_keys, :], ones], axis=1)
        for j in range(group):
            q = q_all[pl.ds(pl.multiple_of(row0, size), size), j * HEAD_DIM:(j + 1) * HEAD_DIM]
            at = pl.ds(pl.multiple_of(j * plane_rows + row0, size), size)
            score = lax.dot_general(
                q, keys, (((1,), (1,)), ((), ())), preferred_element_type=jnp.float32
            )
            if first:
                row = lax.broadcasted_iota(jnp.int32, score.shape, 0) + (count - size)
                col = lax.broadcasted_iota(jnp.int32, score.shape, 1)
                score = jnp.where(col <= row, score, NEG)
            top = jnp.broadcast_to(jnp.max(score, axis=1, keepdims=True), (size, HEAD_DIM))
            if not first:
                before = largest[at, :]
                top = jnp.maximum(before, top)
            spread = jnp.concatenate([top] * (count // HEAD_DIM), axis=1)
            weight = jnp.exp2((score - spread) * scale).astype(jnp.bfloat16)
            product = jnp.dot(weight, values, preferred_element_type=jnp.float32)
            if first:
                summed[at, :] = product
            else:
                shrink = jnp.exp2((before - top) * scale)
                summed[at, :] = summed[at, :] * jnp.concatenate([shrink, shrink], axis=1) + product
            largest[at, :] = top

    def own_tile(shift):
        for r in range(chunks):

            @pl.when(nearest(shift) == r)
            def _(r=r):
                at_keys = pl.ds(pl.multiple_of(plane * plane_rows, plane_rows), (r + 1) * chunk)
                attend(at_keys, r * chunk, chunk, first=True)

    if turns:

        @pl.when(leads)
        def _():
            lax.fori_loop(1, plane + 1, forward, 0)

            @pl.when(plane == 1)
            def _():
                lead_sent(0, chunks)
                pass_turn()

        @pl.when(trails)
        def _():
            @pl.when(plane == 1)
            def _():
                take_turn()
                forward(1, 0)

            @pl.when(plane > 1)
            def _():
                receive(chunk_of(1, 0))

    else:
        lax.fori_loop(1, ahead + 1, forward, 0)

    wait_all(kv_all.at[:, plane_of(plane)], kv_recv)
    wait_all(q_all.at[piece(near)], q_recv.at[near])
    own_tile(0)

    if turns:

        @pl.when(trails & (plane > 1))
        def _():
            take_turn()
            for c in range(1, chunks):
                receive(chunk_of(1, c))
            lax.fori_loop(2, plane, forward, 0)
            for c in range(chunks - 1):
                receive(chunk_of(plane, c))

    for shift in range(1, chunks):
        wait_all(q_all.at[piece(nearest(shift))], q_recv.at[nearest(shift)])
        own_tile(shift)

    if turns:

        @pl.when(leads & (plane > 1))
        def _():
            lead_sent(0, 1)
            pass_turn()

        @pl.when(trails & (plane > 1))
        def _():
            receive(chunk_of(plane, chunks - 1))

    def arrive(step, c):
        @pl.when(step > ahead)
        def _():
            receive(chunk_of(step, c))

    def whole_step(step, carry):
        for c in range(chunks):
            arrive(step, c)
        for row0 in range(0, plane_rows, chunk):
            attend(plane_of(plane - step), row0, chunk)
        return carry

    lax.fori_loop(1, plane, whole_step, 0)

    final = piece(chunk_of(plane, chunks - 1))

    @pl.when(has_down)
    def _():
        for c in range(chunks - 1):
            arrive(plane, c)
            for r in range(chunks):
                attend(piece(chunk_of(plane, c)), r * chunk, chunk)
        arrive(plane, chunks - 1)

    def finish(g):
        for j in range(group):
            at = pl.ds(pl.multiple_of(j * plane_rows + g * rows, rows), rows)
            result[block(g), j * HEAD_DIM:(j + 1) * HEAD_DIM] = (
                summed[at, :HEAD_DIM] / summed[at, HEAD_DIM:]
            ).astype(jnp.bfloat16)

    def close(attending):
        for shift in reversed(range(chunks)):
            for s in range(0, chunk, sub):
                row0 = nearest(shift) * chunk + s
                if attending:
                    attend(final, row0, sub)
                for i in range(per_sub):
                    to = row0 // rows + (me + 1 + i) % per_sub
                    finish(to)

                    @pl.when(to != me)
                    def _(to=to):
                        out_copy(me, to, to).start()

    @pl.when(has_down)
    def _():
        close(True)

    @pl.when(plane == 0)
    def _():
        close(False)

    pltpu.make_async_copy(result.at[block(me)], out_ref.at[:, cols(me, width)], out_recv).start()

    others = (members - 1) * HEAD_DIM
    kv_sent = kv_stage.at[:, :, :others]
    q_sent = q_stage.at[:, :group * others]
    wait_all(kv_sent, kv_send)
    wait_all(q_sent, q_send)

    @pl.when(has_up)
    def _():
        def sent(index, carry):
            @pl.when((index != chunk_of(plane, 0)) | jnp.logical_not(leads & (plane > 1)))
            def _():
                up_copy(index).wait_send()

            return carry

        done = jnp.where(leads & (plane == 1), chunks, 0) if turns else 0
        lax.fori_loop(done, plane * chunks, sent, 0)
        wait_all(kv_stage, rise_send)

    wait_all(result.at[:(members - 1) * rows], out_send)
    wait_all(out_ref, out_recv)


def solution(mesh):
    heads, seqs = mesh.shape["head"], mesh.shape["seq"]

    def on_device(queries, keys, values):
        rows = queries.shape[0]
        members = keys.shape[1] // HEAD_DIM
        inner = members // heads
        planes = seqs // inner
        group = queries.shape[1] // keys.shape[1]
        plane_rows = members * rows
        chunk = math.gcd(plane_rows, TILE)
        total = planes * plane_rows
        chunks = plane_rows // chunk
        relayed = max(planes - 2, 1) * chunks
        raised = max(planes - 1, 1) * chunks
        dma = pltpu.SemaphoreType.DMA
        cfg = (heads, planes, inner, group, rows, chunk)
        return pl.pallas_call(
            functools.partial(kernel, cfg),
            out_shape=pltpu.VMEM(queries.shape, jnp.bfloat16),
            in_specs=[pl.BlockSpec(memory_space=pl.ANY)] * 3,
            out_specs=pl.BlockSpec(memory_space=pltpu.VMEM),
            scratch_shapes=[
                pltpu.VMEM(queries.shape, jnp.bfloat16),
                pltpu.VMEM((2,) + keys.shape, jnp.bfloat16),
                pltpu.VMEM((plane_rows, group * HEAD_DIM), jnp.bfloat16),
                pltpu.VMEM((2, total, HEAD_DIM), jnp.bfloat16),
                pltpu.VMEM((group * plane_rows, HEAD_DIM), jnp.float32),
                pltpu.VMEM((group * plane_rows, 2 * HEAD_DIM), jnp.float32),
                pltpu.VMEM((plane_rows, group * HEAD_DIM), jnp.bfloat16),
                dma((2,)),
                pltpu.SemaphoreType.REGULAR,
                dma(()),
                dma(()),
                dma(()),
                dma((chunks,)),
                dma(()),
                dma((relayed,)),
                dma((raised,)),
                dma(()),
                dma(()),
            ],
            compiler_params=pltpu.CompilerParams(collective_id=0, has_side_effects=True),
        )(queries, keys, values)

    spec = P(("seq", "head"), None)
    return jax.shard_map(
        on_device, mesh=mesh, in_specs=(spec, spec, spec), out_specs=spec, check_vma=False
    )
```

```python
import functools
import math

import jax
import jax.numpy as jnp
from jax import lax
from jax.experimental import pallas as pl
from jax.experimental.pallas import tpu as pltpu
from jax.sharding import PartitionSpec as P

HEAD_DIM = 128
TILE = 256
MESH = pl.DeviceIdType.MESH
NEG = -1e30


def kernel(
    cfg, q_in, k_in, v_in, out_ref, q_stage, kv_stage, q_all, kv_all, largest, summed, result,
    load_sem, go_sem, kv_send, kv_recv, q_send, q_recv, rise_send, up_send, up_recv, out_send, out_recv,
):
    heads, planes, inner, group, rows, chunk = cfg
    members = heads * inner
    plane_rows = members * rows
    chunks = plane_rows // chunk
    per_chunk = members // chunks
    width = group * HEAD_DIM
    seq = lax.axis_index("seq")
    head = lax.axis_index("head")
    plane = seq // inner
    me = (seq % inner) * heads + head
    near = me // per_chunk
    has_up = plane < planes - 1
    has_down = plane > 0

    def member(g):
        return {"head": g % heads, "seq": plane * inner + g // heads}

    def other_plane(step, g=me):
        return {"head": g % heads, "seq": (plane + step) * inner + g // heads}

    turns = inner % 2 == 0
    core = seq % 2 if turns else 0

    def flip(mask, start=me):
        g, bit = start, 1
        while bit < members:
            if mask & bit:
                g = g + bit * (1 - 2 * ((start // bit) % 2))
            bit *= 2
        return g

    def cols(g, size):
        return pl.ds(pl.multiple_of(g * size, HEAD_DIM), size)

    def block(g):
        return pl.ds(pl.multiple_of(g * rows, rows), rows)

    def position(g):
        return pl.ds(pl.multiple_of((plane * members + g) * rows, rows), rows)

    def plane_of(index):
        return pl.ds(pl.multiple_of(index * plane_rows, plane_rows), plane_rows)

    def piece(index):
        return pl.ds(pl.multiple_of(index * chunk, chunk), chunk)

    loads = [
        pltpu.make_async_copy(k_in, kv_stage.at[0], load_sem.at[0]),
        pltpu.make_async_copy(v_in, kv_stage.at[1], load_sem.at[0]),
        pltpu.make_async_copy(q_in, q_stage, load_sem.at[1]),
    ]
    own = [
        pltpu.make_async_copy(k_in.at[:, cols(me, HEAD_DIM)], kv_all.at[0, position(me)], kv_recv),
        pltpu.make_async_copy(v_in.at[:, cols(me, HEAD_DIM)], kv_all.at[1, position(me)], kv_recv),
        pltpu.make_async_copy(q_in.at[:, cols(me, width)], q_all.at[block(me)], q_recv.at[near]),
    ]
    for copy in loads + own:
        copy.start()

    barrier = pltpu.get_barrier_semaphore()
    for d in range(1, members):
        pl.semaphore_signal(
            barrier, inc=1, device_id=member((me + d) % members), device_id_type=MESH
        )

    @pl.when(has_down)
    def _():
        for g in range(members):
            pl.semaphore_signal(barrier, inc=1, device_id=other_plane(-1, g), device_id_type=MESH)

    above = jnp.minimum(planes - 1 - plane, 1)
    pl.semaphore_wait(barrier, members - 1 + above * members)

    def kv_copy(src, dst, to):
        return pltpu.make_async_remote_copy(
            src_ref=kv_stage.at[:, :, cols(dst, HEAD_DIM)],
            dst_ref=kv_all.at[:, position(src)],
            send_sem=kv_send,
            recv_sem=kv_recv,
            device_id=member(to),
            device_id_type=MESH,
        )

    def q_copy(src, dst, to):
        return pltpu.make_async_remote_copy(
            src_ref=q_stage.at[:, cols(dst, width)],
            dst_ref=q_all.at[block(src)],
            send_sem=q_send,
            recv_sem=q_recv.at[src // per_chunk],
            device_id=member(to),
            device_id_type=MESH,
        )

    def up_copy(index):
        return pltpu.make_async_remote_copy(
            src_ref=kv_all.at[:, piece(index)],
            dst_ref=kv_all.at[:, piece(index)],
            send_sem=up_send.at[index],
            recv_sem=up_recv.at[index],
            device_id=other_plane(1),
            device_id_type=MESH,
        )

    def rise_copy(dst):
        return pltpu.make_async_remote_copy(
            src_ref=kv_stage.at[:, :, cols(dst, HEAD_DIM)],
            dst_ref=kv_all.at[:, position(me)],
            send_sem=rise_send,
            recv_sem=up_recv.at[plane * chunks + near],
            device_id=other_plane(1, dst),
            device_id_type=MESH,
        )

    def out_copy(src, dst, to):
        return pltpu.make_async_remote_copy(
            src_ref=result.at[block(dst)],
            dst_ref=out_ref.at[:, cols(src, width)],
            send_sem=out_send,
            recv_sem=out_recv,
            device_id=member(to),
            device_id_type=MESH,
        )

    base = me - core * heads

    def peer(mask):
        return flip(mask, base)

    def reach(mask):
        g = mask // heads
        return (mask % heads > 0) + 2 * (g // (2 if turns else 1) > 0)

    core_of = {m: (m // heads) % 2 if turns else 0 for m in range(members)}
    far_first = sorted(range(members), key=lambda m: (core_of[m], -reach(m), m))
    near_first = sorted(range(members), key=lambda m: (core_of[m], reach(m), m))

    def start_all(copy_of, order):
        for to in map(peer, order):

            @pl.when(to != me)
            def _(to=to):
                copy_of(me, to, to).start()

    def wait_all(ref, sem):
        pltpu.make_async_copy(ref, ref, sem).wait()

    wait_all(kv_stage, load_sem.at[0])
    wait_all(q_stage, load_sem.at[1])

    for side in range(1 + max(core_of.values())):
        start_all(kv_copy, [m for m in far_first if core_of[m] == side])

        @pl.when(has_up)
        def _(side=side):
            for mask in far_first:
                if core_of[mask] == side:
                    rise_copy(peer(mask)).start()

        start_all(q_copy, [m for m in near_first if core_of[m] == side])

    def receive(index):
        wait_all(kv_all.at[:, piece(index)], up_recv.at[index])

        @pl.when(has_up)
        def _():
            up_copy(index).start()

    def nearest(c):
        return (near + c) % chunks

    def chunk_of(step, c):
        return (plane - step) * chunks + nearest(c)

    ahead = jnp.minimum(plane, 1)
    if turns:
        ahead = plane
    ahead = jnp.where(has_up, ahead, 0)

    def forward(step, carry):
        for c in range(chunks):
            receive(chunk_of(step, c))
        return carry

    relays = has_up & has_down
    leads = relays & (core == 0) & turns
    trails = relays & (core == 1) & turns

    def lead_sent(first, last):
        for c in range(first, last):
            up_copy(chunk_of(plane, c)).wait_send()

    def pass_turn():
        sibling = {"head": head, "seq": seq + 1}
        pl.semaphore_signal(go_sem, inc=1, device_id=sibling, device_id_type=MESH)

    def take_turn():
        pl.semaphore_wait(go_sem, 1)

    scale = math.log2(math.e) / math.sqrt(HEAD_DIM)
    sub = chunk // 2 if chunk >= 2 * HEAD_DIM else chunk
    per_sub = sub // rows

    def attend(at_keys, row0, size, first=False):
        keys = kv_all[0, at_keys, :]
        count = keys.shape[0]
        ones = jnp.ones((count, HEAD_DIM), jnp.bfloat16)
        values = jnp.concatenate([kv_all[1, at_keys, :], ones], axis=1)
        for j in range(group):
            q = q_all[pl.ds(pl.multiple_of(row0, size), size), j * HEAD_DIM:(j + 1) * HEAD_DIM]
            at = pl.ds(pl.multiple_of(j * plane_rows + row0, size), size)
            score = lax.dot_general(
                q, keys, (((1,), (1,)), ((), ())), preferred_element_type=jnp.float32
            )
            if first:
                row = lax.broadcasted_iota(jnp.int32, score.shape, 0) + (count - size)
                col = lax.broadcasted_iota(jnp.int32, score.shape, 1)
                score = jnp.where(col <= row, score, NEG)
            top = jnp.broadcast_to(jnp.max(score, axis=1, keepdims=True), (size, HEAD_DIM))
            if not first:
                before = largest[at, :]
                top = jnp.maximum(before, top)
            spread = jnp.concatenate([top] * (count // HEAD_DIM), axis=1)
            weight = jnp.exp2((score - spread) * scale).astype(jnp.bfloat16)
            product = jnp.dot(weight, values, preferred_element_type=jnp.float32)
            if first:
                summed[at, :] = product
            else:
                shrink = jnp.exp2((before - top) * scale)
                summed[at, :] = summed[at, :] * jnp.concatenate([shrink, shrink], axis=1) + product
            largest[at, :] = top

    def own_tile(shift):
        for r in range(chunks):

            @pl.when(nearest(shift) == r)
            def _(r=r):
                at_keys = pl.ds(pl.multiple_of(plane * plane_rows, plane_rows), (r + 1) * chunk)
                attend(at_keys, r * chunk, chunk, first=True)

    if turns:

        @pl.when(leads)
        def _():
            lax.fori_loop(1, plane + 1, forward, 0)

            @pl.when(plane == 1)
            def _():
                lead_sent(0, chunks)
                pass_turn()

        @pl.when(trails)
        def _():
            @pl.when(plane == 1)
            def _():
                take_turn()
                forward(1, 0)

            @pl.when(plane > 1)
            def _():
                receive(chunk_of(1, 0))

    else:
        lax.fori_loop(1, ahead + 1, forward, 0)

    wait_all(kv_all.at[:, plane_of(plane)], kv_recv)
    wait_all(q_all.at[piece(near)], q_recv.at[near])
    own_tile(0)

    if turns:

        @pl.when(trails & (plane > 1))
        def _():
            take_turn()
            for c in range(1, chunks):
                receive(chunk_of(1, c))
            lax.fori_loop(2, plane, forward, 0)
            for c in range(chunks - 1):
                receive(chunk_of(plane, c))

    for shift in range(1, chunks):
        wait_all(q_all.at[piece(nearest(shift))], q_recv.at[nearest(shift)])
        own_tile(shift)

    if turns:

        @pl.when(leads & (plane > 1))
        def _():
            lead_sent(0, 1)
            pass_turn()

        @pl.when(trails & (plane > 1))
        def _():
            receive(chunk_of(plane, chunks - 1))

    def arrive(step, c):
        @pl.when(step > ahead)
        def _():
            receive(chunk_of(step, c))

    def whole_step(step, carry):
        for c in range(chunks):
            arrive(step, c)
        for row0 in range(0, plane_rows, chunk):
            attend(plane_of(plane - step), row0, chunk)
        return carry

    lax.fori_loop(1, plane, whole_step, 0)

    final = piece(chunk_of(plane, chunks - 1))

    @pl.when(has_down)
    def _():
        for c in range(chunks - 1):
            arrive(plane, c)
            for r in range(chunks):
                attend(piece(chunk_of(plane, c)), r * chunk, chunk)
        arrive(plane, chunks - 1)

    def finish(g):
        for j in range(group):
            at = pl.ds(pl.multiple_of(j * plane_rows + g * rows, rows), rows)
            result[block(g), j * HEAD_DIM:(j + 1) * HEAD_DIM] = (
                summed[at, :HEAD_DIM] / summed[at, HEAD_DIM:]
            ).astype(jnp.bfloat16)

    def close(attending):
        for shift in reversed(range(chunks)):
            size = chunk if shift else chunk
            for s in range(0, chunk, size):
                row0 = nearest(shift) * chunk + s
                if attending:
                    attend(final, row0, size)
                for i in range(size // rows):
                    to = row0 // rows + (me + 1 + i) % (size // rows)
                    finish(to)
                    if shift:
                        out_copy(me, to, to).start()
                        continue

                    @pl.when(to != me)
                    def _(to=to):
                        out_copy(me, to, to).start()

    @pl.when(has_down)
    def _():
        close(True)

    @pl.when(plane == 0)
    def _():
        close(False)

    pltpu.make_async_copy(result.at[block(me)], out_ref.at[:, cols(me, width)], out_recv).start()

    others = (members - 1) * HEAD_DIM
    kv_sent = kv_stage.at[:, :, :others]
    q_sent = q_stage.at[:, :group * others]
    wait_all(kv_sent, kv_send)
    wait_all(q_sent, q_send)

    @pl.when(has_up)
    def _():
        def sent(index, carry):
            @pl.when((index != chunk_of(plane, 0)) | jnp.logical_not(leads & (plane > 1)))
            def _():
                up_copy(index).wait_send()

            return carry

        done = jnp.where(leads & (plane == 1), chunks, 0) if turns else 0
        lax.fori_loop(done, plane * chunks, sent, 0)
        wait_all(kv_stage, rise_send)

    wait_all(result.at[:(members - 1) * rows], out_send)
    wait_all(out_ref, out_recv)


def solution(mesh):
    heads, seqs = mesh.shape["head"], mesh.shape["seq"]

    def on_device(queries, keys, values):
        rows = queries.shape[0]
        members = keys.shape[1] // HEAD_DIM
        inner = members // heads
        planes = seqs // inner
        group = queries.shape[1] // keys.shape[1]
        plane_rows = members * rows
        chunk = math.gcd(plane_rows, TILE)
        total = planes * plane_rows
        chunks = plane_rows // chunk
        relayed = max(planes - 2, 1) * chunks
        raised = max(planes - 1, 1) * chunks
        dma = pltpu.SemaphoreType.DMA
        cfg = (heads, planes, inner, group, rows, chunk)
        return pl.pallas_call(
            functools.partial(kernel, cfg),
            out_shape=pltpu.VMEM(queries.shape, jnp.bfloat16),
            in_specs=[pl.BlockSpec(memory_space=pl.ANY)] * 3,
            out_specs=pl.BlockSpec(memory_space=pltpu.VMEM),
            scratch_shapes=[
                pltpu.VMEM(queries.shape, jnp.bfloat16),
                pltpu.VMEM((2,) + keys.shape, jnp.bfloat16),
                pltpu.VMEM((plane_rows, group * HEAD_DIM), jnp.bfloat16),
                pltpu.VMEM((2, total, HEAD_DIM), jnp.bfloat16),
                pltpu.VMEM((group * plane_rows, HEAD_DIM), jnp.float32),
                pltpu.VMEM((group * plane_rows, 2 * HEAD_DIM), jnp.float32),
                pltpu.VMEM((plane_rows, group * HEAD_DIM), jnp.bfloat16),
                dma((2,)),
                pltpu.SemaphoreType.REGULAR,
                dma(()),
                dma(()),
                dma(()),
                dma((chunks,)),
                dma(()),
                dma((relayed,)),
                dma((raised,)),
                dma(()),
                dma(()),
            ],
            compiler_params=pltpu.CompilerParams(collective_id=0, has_side_effects=True),
        )(queries, keys, values)

    spec = P(("seq", "head"), None)
    return jax.shard_map(
        on_device, mesh=mesh, in_specs=(spec, spec, spec), out_specs=spec, check_vma=False
    )
```

```python
import functools
import math

import jax
import jax.numpy as jnp
from jax import lax
from jax.experimental import pallas as pl
from jax.experimental.pallas import tpu as pltpu
from jax.sharding import PartitionSpec as P

HEAD_DIM = 128
TILE = 256
MESH = pl.DeviceIdType.MESH
NEG = -1e30


def kernel(
    cfg, q_in, k_in, v_in, out_ref, q_stage, kv_stage, q_all, kv_all, largest, summed, result,
    load_sem, go_sem, kv_send, kv_recv, q_send, q_recv, rise_send, up_send, up_recv, out_send, out_recv,
):
    heads, planes, inner, group, rows, chunk = cfg
    members = heads * inner
    plane_rows = members * rows
    chunks = plane_rows // chunk
    per_chunk = members // chunks
    width = group * HEAD_DIM
    seq = lax.axis_index("seq")
    head = lax.axis_index("head")
    plane = seq // inner
    me = (seq % inner) * heads + head
    near = me // per_chunk
    has_up = plane < planes - 1
    has_down = plane > 0

    def member(g):
        return {"head": g % heads, "seq": plane * inner + g // heads}

    def other_plane(step, g=me):
        return {"head": g % heads, "seq": (plane + step) * inner + g // heads}

    turns = inner % 2 == 0
    core = seq % 2 if turns else 0

    def flip(mask, start=me):
        g, bit = start, 1
        while bit < members:
            if mask & bit:
                g = g + bit * (1 - 2 * ((start // bit) % 2))
            bit *= 2
        return g

    def cols(g, size):
        return pl.ds(pl.multiple_of(g * size, HEAD_DIM), size)

    def block(g):
        return pl.ds(pl.multiple_of(g * rows, rows), rows)

    def position(g):
        return pl.ds(pl.multiple_of((plane * members + g) * rows, rows), rows)

    def plane_of(index):
        return pl.ds(pl.multiple_of(index * plane_rows, plane_rows), plane_rows)

    def piece(index):
        return pl.ds(pl.multiple_of(index * chunk, chunk), chunk)

    loads = [
        pltpu.make_async_copy(k_in, kv_stage.at[0], load_sem.at[0]),
        pltpu.make_async_copy(v_in, kv_stage.at[1], load_sem.at[0]),
        pltpu.make_async_copy(q_in, q_stage, load_sem.at[1]),
    ]
    own = [
        pltpu.make_async_copy(k_in.at[:, cols(me, HEAD_DIM)], kv_all.at[0, position(me)], kv_recv),
        pltpu.make_async_copy(v_in.at[:, cols(me, HEAD_DIM)], kv_all.at[1, position(me)], kv_recv),
        pltpu.make_async_copy(q_in.at[:, cols(me, width)], q_all.at[block(me)], q_recv.at[near]),
    ]
    barrier = pltpu.get_barrier_semaphore()
    @pl.when(has_down)
    def _():
        for g in range(members):
            pl.semaphore_signal(barrier, inc=1, device_id=other_plane(-1, g), device_id_type=MESH)

    for d in range(1, members):
        pl.semaphore_signal(
            barrier, inc=1, device_id=member((me + d) % members), device_id_type=MESH
        )

    for copy in loads + own:
        copy.start()

    above = jnp.minimum(planes - 1 - plane, 1)
    pl.semaphore_wait(barrier, members - 1 + above * members)

    def kv_copy(src, dst, to):
        return pltpu.make_async_remote_copy(
            src_ref=kv_stage.at[:, :, cols(dst, HEAD_DIM)],
            dst_ref=kv_all.at[:, position(src)],
            send_sem=kv_send,
            recv_sem=kv_recv,
            device_id=member(to),
            device_id_type=MESH,
        )

    def q_copy(src, dst, to):
        return pltpu.make_async_remote_copy(
            src_ref=q_stage.at[:, cols(dst, width)],
            dst_ref=q_all.at[block(src)],
            send_sem=q_send,
            recv_sem=q_recv.at[src // per_chunk],
            device_id=member(to),
            device_id_type=MESH,
        )

    def up_copy(index):
        return pltpu.make_async_remote_copy(
            src_ref=kv_all.at[:, piece(index)],
            dst_ref=kv_all.at[:, piece(index)],
            send_sem=up_send.at[index],
            recv_sem=up_recv.at[index],
            device_id=other_plane(1),
            device_id_type=MESH,
        )

    def rise_copy(dst):
        return pltpu.make_async_remote_copy(
            src_ref=kv_stage.at[:, :, cols(dst, HEAD_DIM)],
            dst_ref=kv_all.at[:, position(me)],
            send_sem=rise_send,
            recv_sem=up_recv.at[plane * chunks + near],
            device_id=other_plane(1, dst),
            device_id_type=MESH,
        )

    def out_copy(src, dst, to):
        return pltpu.make_async_remote_copy(
            src_ref=result.at[block(dst)],
            dst_ref=out_ref.at[:, cols(src, width)],
            send_sem=out_send,
            recv_sem=out_recv,
            device_id=member(to),
            device_id_type=MESH,
        )

    base = me - core * heads

    def peer(mask):
        return flip(mask, base)

    def reach(mask):
        g = mask // heads
        return (mask % heads > 0) + 2 * (g // (2 if turns else 1) > 0)

    core_of = {m: (m // heads) % 2 if turns else 0 for m in range(members)}
    far_first = sorted(range(members), key=lambda m: (core_of[m], -reach(m), m))
    near_first = sorted(range(members), key=lambda m: (core_of[m], reach(m), m))

    def start_all(copy_of, order):
        for to in map(peer, order):

            @pl.when(to != me)
            def _(to=to):
                copy_of(me, to, to).start()

    def wait_all(ref, sem):
        pltpu.make_async_copy(ref, ref, sem).wait()

    wait_all(kv_stage, load_sem.at[0])
    wait_all(q_stage, load_sem.at[1])

    for side in range(1 + max(core_of.values())):
        start_all(kv_copy, [m for m in far_first if core_of[m] == side])

        @pl.when(has_up)
        def _(side=side):
            for mask in far_first:
                if core_of[mask] == side:
                    rise_copy(peer(mask)).start()

        start_all(q_copy, [m for m in near_first if core_of[m] == side])

    def receive(index):
        wait_all(kv_all.at[:, piece(index)], up_recv.at[index])

        @pl.when(has_up)
        def _():
            up_copy(index).start()

    def nearest(c):
        return (near + c) % chunks

    def chunk_of(step, c):
        return (plane - step) * chunks + nearest(c)

    ahead = jnp.minimum(plane, 1)
    if turns:
        ahead = plane
    ahead = jnp.where(has_up, ahead, 0)

    def forward(step, carry):
        for c in range(chunks):
            receive(chunk_of(step, c))
        return carry

    relays = has_up & has_down
    leads = relays & (core == 0) & turns
    trails = relays & (core == 1) & turns

    def lead_sent(first, last):
        for c in range(first, last):
            up_copy(chunk_of(plane, c)).wait_send()

    def pass_turn():
        sibling = {"head": head, "seq": seq + 1}
        pl.semaphore_signal(go_sem, inc=1, device_id=sibling, device_id_type=MESH)

    def take_turn():
        pl.semaphore_wait(go_sem, 1)

    scale = math.log2(math.e) / math.sqrt(HEAD_DIM)
    sub = chunk // 2 if chunk >= 2 * HEAD_DIM else chunk
    per_sub = sub // rows

    def attend(at_keys, row0, size, first=False):
        keys = kv_all[0, at_keys, :]
        count = keys.shape[0]
        ones = jnp.ones((count, HEAD_DIM), jnp.bfloat16)
        values = jnp.concatenate([kv_all[1, at_keys, :], ones], axis=1)
        for j in range(group):
            q = q_all[pl.ds(pl.multiple_of(row0, size), size), j * HEAD_DIM:(j + 1) * HEAD_DIM]
            at = pl.ds(pl.multiple_of(j * plane_rows + row0, size), size)
            score = lax.dot_general(
                q, keys, (((1,), (1,)), ((), ())), preferred_element_type=jnp.float32
            )
            if first:
                row = lax.broadcasted_iota(jnp.int32, score.shape, 0) + (count - size)
                col = lax.broadcasted_iota(jnp.int32, score.shape, 1)
                score = jnp.where(col <= row, score, NEG)
            top = jnp.broadcast_to(jnp.max(score, axis=1, keepdims=True), (size, HEAD_DIM))
            if not first:
                before = largest[at, :]
                top = jnp.maximum(before, top)
            spread = jnp.concatenate([top] * (count // HEAD_DIM), axis=1)
            weight = jnp.exp2((score - spread) * scale).astype(jnp.bfloat16)
            product = jnp.dot(weight, values, preferred_element_type=jnp.float32)
            if first:
                summed[at, :] = product
            else:
                shrink = jnp.exp2((before - top) * scale)
                summed[at, :] = summed[at, :] * jnp.concatenate([shrink, shrink], axis=1) + product
            largest[at, :] = top

    def own_tile(shift):
        for r in range(chunks):

            @pl.when(nearest(shift) == r)
            def _(r=r):
                at_keys = pl.ds(pl.multiple_of(plane * plane_rows, plane_rows), (r + 1) * chunk)
                attend(at_keys, r * chunk, chunk, first=True)

    if turns:

        @pl.when(leads)
        def _():
            lax.fori_loop(1, plane + 1, forward, 0)

            @pl.when(plane == 1)
            def _():
                lead_sent(0, chunks)
                pass_turn()

        @pl.when(trails)
        def _():
            @pl.when(plane == 1)
            def _():
                take_turn()
                forward(1, 0)

            @pl.when(plane > 1)
            def _():
                receive(chunk_of(1, 0))

    else:
        lax.fori_loop(1, ahead + 1, forward, 0)

    wait_all(kv_all.at[:, plane_of(plane)], kv_recv)
    wait_all(q_all.at[piece(near)], q_recv.at[near])
    own_tile(0)

    if turns:

        @pl.when(trails & (plane > 1))
        def _():
            take_turn()
            for c in range(1, chunks):
                receive(chunk_of(1, c))
            lax.fori_loop(2, plane, forward, 0)
            for c in range(chunks - 1):
                receive(chunk_of(plane, c))

    for shift in range(1, chunks):
        wait_all(q_all.at[piece(nearest(shift))], q_recv.at[nearest(shift)])
        own_tile(shift)

    if turns:

        @pl.when(leads & (plane > 1))
        def _():
            lead_sent(0, 1)
            pass_turn()

        @pl.when(trails & (plane > 1))
        def _():
            receive(chunk_of(plane, chunks - 1))

    def arrive(step, c):
        @pl.when(step > ahead)
        def _():
            receive(chunk_of(step, c))

    def whole_step(step, carry):
        for c in range(chunks):
            arrive(step, c)
        for row0 in range(0, plane_rows, chunk):
            attend(plane_of(plane - step), row0, chunk)
        return carry

    lax.fori_loop(1, plane, whole_step, 0)

    final = piece(chunk_of(plane, chunks - 1))

    @pl.when(has_down)
    def _():
        for c in range(chunks - 1):
            arrive(plane, c)
            for r in range(chunks):
                attend(piece(chunk_of(plane, c)), r * chunk, chunk)
        arrive(plane, chunks - 1)

    def finish(g):
        for j in range(group):
            at = pl.ds(pl.multiple_of(j * plane_rows + g * rows, rows), rows)
            result[block(g), j * HEAD_DIM:(j + 1) * HEAD_DIM] = (
                summed[at, :HEAD_DIM] / summed[at, HEAD_DIM:]
            ).astype(jnp.bfloat16)

    def close(attending):
        for shift in reversed(range(chunks)):
            size = chunk if shift else chunk
            for s in range(0, chunk, size):
                row0 = nearest(shift) * chunk + s
                if attending:
                    attend(final, row0, size)
                for i in range(size // rows):
                    to = row0 // rows + (me + 1 + i) % (size // rows)
                    finish(to)
                    if shift:
                        out_copy(me, to, to).start()
                        continue

                    @pl.when(to != me)
                    def _(to=to):
                        out_copy(me, to, to).start()

    @pl.when(has_down)
    def _():
        close(True)

    @pl.when(plane == 0)
    def _():
        close(False)

    pltpu.make_async_copy(result.at[block(me)], out_ref.at[:, cols(me, width)], out_recv).start()

    others = (members - 1) * HEAD_DIM
    kv_sent = kv_stage.at[:, :, :others]
    q_sent = q_stage.at[:, :group * others]
    wait_all(kv_sent, kv_send)
    wait_all(q_sent, q_send)

    @pl.when(has_up)
    def _():
        def sent(index, carry):
            @pl.when((index != chunk_of(plane, 0)) | jnp.logical_not(leads & (plane > 1)))
            def _():
                up_copy(index).wait_send()

            return carry

        done = jnp.where(leads & (plane == 1), chunks, 0) if turns else 0
        lax.fori_loop(done, plane * chunks, sent, 0)
        wait_all(kv_stage, rise_send)

    wait_all(result.at[:(members - 1) * rows], out_send)
    wait_all(out_ref, out_recv)


def solution(mesh):
    heads, seqs = mesh.shape["head"], mesh.shape["seq"]

    def on_device(queries, keys, values):
        rows = queries.shape[0]
        members = keys.shape[1] // HEAD_DIM
        inner = members // heads
        planes = seqs // inner
        group = queries.shape[1] // keys.shape[1]
        plane_rows = members * rows
        chunk = math.gcd(plane_rows, TILE)
        total = planes * plane_rows
        chunks = plane_rows // chunk
        relayed = max(planes - 2, 1) * chunks
        raised = max(planes - 1, 1) * chunks
        dma = pltpu.SemaphoreType.DMA
        cfg = (heads, planes, inner, group, rows, chunk)
        return pl.pallas_call(
            functools.partial(kernel, cfg),
            out_shape=pltpu.VMEM(queries.shape, jnp.bfloat16),
            in_specs=[pl.BlockSpec(memory_space=pl.ANY)] * 3,
            out_specs=pl.BlockSpec(memory_space=pltpu.VMEM),
            scratch_shapes=[
                pltpu.VMEM(queries.shape, jnp.bfloat16),
                pltpu.VMEM((2,) + keys.shape, jnp.bfloat16),
                pltpu.VMEM((plane_rows, group * HEAD_DIM), jnp.bfloat16),
                pltpu.VMEM((2, total, HEAD_DIM), jnp.bfloat16),
                pltpu.VMEM((group * plane_rows, HEAD_DIM), jnp.float32),
                pltpu.VMEM((group * plane_rows, 2 * HEAD_DIM), jnp.float32),
                pltpu.VMEM((plane_rows, group * HEAD_DIM), jnp.bfloat16),
                dma((2,)),
                pltpu.SemaphoreType.REGULAR,
                dma(()),
                dma(()),
                dma(()),
                dma((chunks,)),
                dma(()),
                dma((relayed,)),
                dma((raised,)),
                dma(()),
                dma(()),
            ],
            compiler_params=pltpu.CompilerParams(collective_id=0, has_side_effects=True),
        )(queries, keys, values)

    spec = P(("seq", "head"), None)
    return jax.shard_map(
        on_device, mesh=mesh, in_specs=(spec, spec, spec), out_specs=spec, check_vma=False
    )
```

```python
import functools
import math

import jax
import jax.numpy as jnp
from jax import lax
from jax.experimental import pallas as pl
from jax.experimental.pallas import tpu as pltpu
from jax.sharding import PartitionSpec as P

HEAD_DIM = 128
TILE = 256
MESH = pl.DeviceIdType.MESH
NEG = -1e30


def kernel(
    cfg, q_in, k_in, v_in, out_ref, q_stage, kv_stage, q_all, kv_all, largest, summed, result,
    load_sem, go_sem, kv_send, kv_recv, q_send, q_recv, rise_send, up_send, up_recv, out_send, out_recv,
):
    heads, planes, inner, group, rows, chunk = cfg
    members = heads * inner
    plane_rows = members * rows
    chunks = plane_rows // chunk
    per_chunk = members // chunks
    width = group * HEAD_DIM
    seq = lax.axis_index("seq")
    head = lax.axis_index("head")
    plane = seq // inner
    me = (seq % inner) * heads + head
    near = me // per_chunk
    has_up = plane < planes - 1
    has_down = plane > 0

    def member(g):
        return {"head": g % heads, "seq": plane * inner + g // heads}

    def other_plane(step, g=me):
        return {"head": g % heads, "seq": (plane + step) * inner + g // heads}

    turns = inner % 2 == 0
    core = seq % 2 if turns else 0

    def flip(mask, start=me):
        g, bit = start, 1
        while bit < members:
            if mask & bit:
                g = g + bit * (1 - 2 * ((start // bit) % 2))
            bit *= 2
        return g

    def cols(g, size):
        return pl.ds(pl.multiple_of(g * size, HEAD_DIM), size)

    def block(g):
        return pl.ds(pl.multiple_of(g * rows, rows), rows)

    def position(g):
        return pl.ds(pl.multiple_of((plane * members + g) * rows, rows), rows)

    def plane_of(index):
        return pl.ds(pl.multiple_of(index * plane_rows, plane_rows), plane_rows)

    def piece(index):
        return pl.ds(pl.multiple_of(index * chunk, chunk), chunk)

    loads = [
        pltpu.make_async_copy(k_in, kv_stage.at[0], load_sem.at[0]),
        pltpu.make_async_copy(v_in, kv_stage.at[1], load_sem.at[0]),
        pltpu.make_async_copy(q_in, q_stage, load_sem.at[1]),
    ]
    own = [
        pltpu.make_async_copy(k_in.at[:, cols(me, HEAD_DIM)], kv_all.at[0, position(me)], kv_recv),
        pltpu.make_async_copy(v_in.at[:, cols(me, HEAD_DIM)], kv_all.at[1, position(me)], kv_recv),
        pltpu.make_async_copy(q_in.at[:, cols(me, width)], q_all.at[block(me)], q_recv.at[near]),
    ]
    for copy in loads + own:
        copy.start()

    barrier = pltpu.get_barrier_semaphore()
    for d in range(1, members):
        pl.semaphore_signal(
            barrier, inc=1, device_id=member((me + d) % members), device_id_type=MESH
        )

    @pl.when(has_down)
    def _():
        for g in range(members):
            pl.semaphore_signal(barrier, inc=1, device_id=other_plane(-1, g), device_id_type=MESH)

    above = jnp.minimum(planes - 1 - plane, 1)
    pl.semaphore_wait(barrier, members - 1 + above * members)

    def kv_copy(src, dst, to):
        return pltpu.make_async_remote_copy(
            src_ref=kv_stage.at[:, :, cols(dst, HEAD_DIM)],
            dst_ref=kv_all.at[:, position(src)],
            send_sem=kv_send,
            recv_sem=kv_recv,
            device_id=member(to),
            device_id_type=MESH,
        )

    def q_copy(src, dst, to):
        return pltpu.make_async_remote_copy(
            src_ref=q_stage.at[:, cols(dst, width)],
            dst_ref=q_all.at[block(src)],
            send_sem=q_send,
            recv_sem=q_recv.at[src // per_chunk],
            device_id=member(to),
            device_id_type=MESH,
        )

    def up_copy(index):
        return pltpu.make_async_remote_copy(
            src_ref=kv_all.at[:, piece(index)],
            dst_ref=kv_all.at[:, piece(index)],
            send_sem=up_send.at[index],
            recv_sem=up_recv.at[index],
            device_id=other_plane(1),
            device_id_type=MESH,
        )

    def rise_copy(dst):
        return pltpu.make_async_remote_copy(
            src_ref=kv_stage.at[:, :, cols(dst, HEAD_DIM)],
            dst_ref=kv_all.at[:, position(me)],
            send_sem=rise_send,
            recv_sem=up_recv.at[plane * chunks + near],
            device_id=other_plane(1, dst),
            device_id_type=MESH,
        )

    def out_copy(src, dst, to):
        return pltpu.make_async_remote_copy(
            src_ref=result.at[block(dst)],
            dst_ref=out_ref.at[:, cols(src, width)],
            send_sem=out_send,
            recv_sem=out_recv,
            device_id=member(to),
            device_id_type=MESH,
        )

    base = me - core * heads

    def peer(mask):
        return flip(mask, base)

    def reach(mask):
        g = mask // heads
        return (mask % heads > 0) + 2 * (g // (2 if turns else 1) > 0)

    core_of = {m: (m // heads) % 2 if turns else 0 for m in range(members)}
    far_first = sorted(range(members), key=lambda m: (core_of[m], -reach(m), m))
    near_first = sorted(range(members), key=lambda m: (core_of[m], reach(m), m))

    def start_all(copy_of, order):
        for to in map(peer, order):

            @pl.when(to != me)
            def _(to=to):
                copy_of(me, to, to).start()

    def wait_all(ref, sem):
        pltpu.make_async_copy(ref, ref, sem).wait()

    wait_all(kv_stage, load_sem.at[0])
    wait_all(q_stage, load_sem.at[1])

    for side in range(1 + max(core_of.values())):
        start_all(kv_copy, [m for m in far_first if core_of[m] == side])

        @pl.when(has_up)
        def _(side=side):
            for mask in far_first:
                if core_of[mask] == side:
                    rise_copy(peer(mask)).start()

        start_all(q_copy, [m for m in near_first if core_of[m] == side])

    def receive(index):
        wait_all(kv_all.at[:, piece(index)], up_recv.at[index])

        @pl.when(has_up)
        def _():
            up_copy(index).start()

    def nearest(c):
        return (near + c) % chunks

    def chunk_of(step, c):
        return (plane - step) * chunks + nearest(c)

    ahead = jnp.minimum(plane, 1)
    if turns:
        ahead = plane
    ahead = jnp.where(has_up, ahead, 0)

    def forward(step, carry):
        for c in range(chunks):
            receive(chunk_of(step, c))
        return carry

    relays = has_up & has_down
    leads = relays & (core == 0) & turns
    trails = relays & (core == 1) & turns

    def lead_sent(first, last):
        for c in range(first, last):
            up_copy(chunk_of(plane, c)).wait_send()

    def pass_turn():
        sibling = {"head": head, "seq": seq + 1}
        pl.semaphore_signal(go_sem, inc=1, device_id=sibling, device_id_type=MESH)

    def take_turn():
        pl.semaphore_wait(go_sem, 1)

    scale = math.log2(math.e) / math.sqrt(HEAD_DIM)
    sub = chunk // 2 if chunk >= 2 * HEAD_DIM else chunk
    per_sub = sub // rows

    def attend(at_keys, row0, size, first=False, closing=False):
        keys = kv_all[0, at_keys, :]
        count = keys.shape[0]
        ones = jnp.ones((count, HEAD_DIM), jnp.bfloat16)
        values = jnp.concatenate([kv_all[1, at_keys, :], ones], axis=1)
        for j in range(group):
            q = q_all[pl.ds(pl.multiple_of(row0, size), size), j * HEAD_DIM:(j + 1) * HEAD_DIM]
            at = pl.ds(pl.multiple_of(j * plane_rows + row0, size), size)
            score = lax.dot_general(
                q, keys, (((1,), (1,)), ((), ())), preferred_element_type=jnp.float32
            )
            if first:
                row = lax.broadcasted_iota(jnp.int32, score.shape, 0) + (count - size)
                col = lax.broadcasted_iota(jnp.int32, score.shape, 1)
                score = jnp.where(col <= row, score, NEG)
            top = jnp.broadcast_to(jnp.max(score, axis=1, keepdims=True), (size, HEAD_DIM))
            if not first:
                before = largest[at, :]
                top = jnp.maximum(before, top)
            spread = jnp.concatenate([top] * (count // HEAD_DIM), axis=1)
            weight = jnp.exp2((score - spread) * scale).astype(jnp.bfloat16)
            product = jnp.dot(weight, values, preferred_element_type=jnp.float32)
            if not first:
                shrink = jnp.exp2((before - top) * scale)
                product = summed[at, :] * jnp.concatenate([shrink, shrink], axis=1) + product
            if closing:
                result[pl.ds(pl.multiple_of(row0, size), size), j * HEAD_DIM:(j + 1) * HEAD_DIM] = (
                    product[:, :HEAD_DIM] / product[:, HEAD_DIM:]
                ).astype(jnp.bfloat16)
            else:
                summed[at, :] = product
                largest[at, :] = top

    def own_tile(shift):
        for r in range(chunks):

            @pl.when(nearest(shift) == r)
            def _(r=r):
                at_keys = pl.ds(pl.multiple_of(plane * plane_rows, plane_rows), (r + 1) * chunk)
                attend(at_keys, r * chunk, chunk, first=True)

    if turns:

        @pl.when(leads)
        def _():
            lax.fori_loop(1, plane + 1, forward, 0)

            @pl.when(plane == 1)
            def _():
                lead_sent(0, chunks)
                pass_turn()

        @pl.when(trails)
        def _():
            @pl.when(plane == 1)
            def _():
                take_turn()
                forward(1, 0)

            @pl.when(plane > 1)
            def _():
                receive(chunk_of(1, 0))

    else:
        lax.fori_loop(1, ahead + 1, forward, 0)

    wait_all(kv_all.at[:, plane_of(plane)], kv_recv)
    wait_all(q_all.at[piece(near)], q_recv.at[near])
    own_tile(0)

    if turns:

        @pl.when(trails & (plane > 1))
        def _():
            take_turn()
            for c in range(1, chunks):
                receive(chunk_of(1, c))
            lax.fori_loop(2, plane, forward, 0)
            for c in range(chunks - 1):
                receive(chunk_of(plane, c))

    for shift in range(1, chunks):
        wait_all(q_all.at[piece(nearest(shift))], q_recv.at[nearest(shift)])
        own_tile(shift)

    if turns:

        @pl.when(leads & (plane > 1))
        def _():
            lead_sent(0, 1)
            pass_turn()

        @pl.when(trails & (plane > 1))
        def _():
            receive(chunk_of(plane, chunks - 1))

    def arrive(step, c):
        @pl.when(step > ahead)
        def _():
            receive(chunk_of(step, c))

    def whole_step(step, carry):
        for c in range(chunks):
            arrive(step, c)
        for row0 in range(0, plane_rows, chunk):
            attend(plane_of(plane - step), row0, chunk)
        return carry

    lax.fori_loop(1, plane, whole_step, 0)

    final = piece(chunk_of(plane, chunks - 1))

    @pl.when(has_down)
    def _():
        for c in range(chunks - 1):
            arrive(plane, c)
            for r in range(chunks):
                attend(piece(chunk_of(plane, c)), r * chunk, chunk)
        arrive(plane, chunks - 1)

    def finish(g):
        for j in range(group):
            at = pl.ds(pl.multiple_of(j * plane_rows + g * rows, rows), rows)
            result[block(g), j * HEAD_DIM:(j + 1) * HEAD_DIM] = (
                summed[at, :HEAD_DIM] / summed[at, HEAD_DIM:]
            ).astype(jnp.bfloat16)

    def close(attending):
        for shift in reversed(range(chunks)):
            size = chunk if shift else chunk
            for s in range(0, chunk, size):
                row0 = nearest(shift) * chunk + s
                if attending:
                    attend(final, row0, size, closing=True)
                for i in range(size // rows):
                    to = row0 // rows + (me + 1 + i) % (size // rows)
                    if not attending:
                        finish(to)
                    if shift:
                        out_copy(me, to, to).start()
                        continue

                    @pl.when(to != me)
                    def _(to=to):
                        out_copy(me, to, to).start()

    @pl.when(has_down)
    def _():
        close(True)

    @pl.when(plane == 0)
    def _():
        close(False)

    pltpu.make_async_copy(result.at[block(me)], out_ref.at[:, cols(me, width)], out_recv).start()

    others = (members - 1) * HEAD_DIM
    kv_sent = kv_stage.at[:, :, :others]
    q_sent = q_stage.at[:, :group * others]
    wait_all(kv_sent, kv_send)
    wait_all(q_sent, q_send)

    @pl.when(has_up)
    def _():
        def sent(index, carry):
            @pl.when((index != chunk_of(plane, 0)) | jnp.logical_not(leads & (plane > 1)))
            def _():
                up_copy(index).wait_send()

            return carry

        done = jnp.where(leads & (plane == 1), chunks, 0) if turns else 0
        lax.fori_loop(done, plane * chunks, sent, 0)
        wait_all(kv_stage, rise_send)

    wait_all(result.at[:(members - 1) * rows], out_send)
    wait_all(out_ref, out_recv)


def solution(mesh):
    heads, seqs = mesh.shape["head"], mesh.shape["seq"]

    def on_device(queries, keys, values):
        rows = queries.shape[0]
        members = keys.shape[1] // HEAD_DIM
        inner = members // heads
        planes = seqs // inner
        group = queries.shape[1] // keys.shape[1]
        plane_rows = members * rows
        chunk = math.gcd(plane_rows, TILE)
        total = planes * plane_rows
        chunks = plane_rows // chunk
        relayed = max(planes - 2, 1) * chunks
        raised = max(planes - 1, 1) * chunks
        dma = pltpu.SemaphoreType.DMA
        cfg = (heads, planes, inner, group, rows, chunk)
        return pl.pallas_call(
            functools.partial(kernel, cfg),
            out_shape=pltpu.VMEM(queries.shape, jnp.bfloat16),
            in_specs=[pl.BlockSpec(memory_space=pl.ANY)] * 3,
            out_specs=pl.BlockSpec(memory_space=pltpu.VMEM),
            scratch_shapes=[
                pltpu.VMEM(queries.shape, jnp.bfloat16),
                pltpu.VMEM((2,) + keys.shape, jnp.bfloat16),
                pltpu.VMEM((plane_rows, group * HEAD_DIM), jnp.bfloat16),
                pltpu.VMEM((2, total, HEAD_DIM), jnp.bfloat16),
                pltpu.VMEM((group * plane_rows, HEAD_DIM), jnp.float32),
                pltpu.VMEM((group * plane_rows, 2 * HEAD_DIM), jnp.float32),
                pltpu.VMEM((plane_rows, group * HEAD_DIM), jnp.bfloat16),
                dma((2,)),
                pltpu.SemaphoreType.REGULAR,
                dma(()),
                dma(()),
                dma(()),
                dma((chunks,)),
                dma(()),
                dma((relayed,)),
                dma((raised,)),
                dma(()),
                dma(()),
            ],
            compiler_params=pltpu.CompilerParams(collective_id=0, has_side_effects=True),
        )(queries, keys, values)

    spec = P(("seq", "head"), None)
    return jax.shard_map(
        on_device, mesh=mesh, in_specs=(spec, spec, spec), out_specs=spec, check_vma=False
    )
```

```python
import functools
import math

import jax
import jax.numpy as jnp
from jax import lax
from jax.experimental import pallas as pl
from jax.experimental.pallas import tpu as pltpu
from jax.sharding import PartitionSpec as P

HEAD_DIM = 128
TILE = 256
MESH = pl.DeviceIdType.MESH
NEG = -1e30


def kernel(
    cfg, q_in, k_in, v_in, out_ref, q_stage, kv_stage, q_all, kv_all, largest, summed, result,
    load_sem, go_sem, kv_send, kv_recv, q_send, q_recv, rise_send, up_send, up_recv, out_send, out_recv,
):
    heads, planes, inner, group, rows, chunk = cfg
    members = heads * inner
    plane_rows = members * rows
    chunks = plane_rows // chunk
    per_chunk = members // chunks
    width = group * HEAD_DIM
    seq = lax.axis_index("seq")
    head = lax.axis_index("head")
    plane = seq // inner
    me = (seq % inner) * heads + head
    near = me // per_chunk
    has_up = plane < planes - 1
    has_down = plane > 0

    def member(g):
        return {"head": g % heads, "seq": plane * inner + g // heads}

    def other_plane(step, g=me):
        return {"head": g % heads, "seq": (plane + step) * inner + g // heads}

    turns = inner % 2 == 0
    core = seq % 2 if turns else 0

    def flip(mask, start=me):
        g, bit = start, 1
        while bit < members:
            if mask & bit:
                g = g + bit * (1 - 2 * ((start // bit) % 2))
            bit *= 2
        return g

    def cols(g, size):
        return pl.ds(pl.multiple_of(g * size, HEAD_DIM), size)

    def block(g):
        return pl.ds(pl.multiple_of(g * rows, rows), rows)

    def position(g):
        return pl.ds(pl.multiple_of((plane * members + g) * rows, rows), rows)

    def plane_of(index):
        return pl.ds(pl.multiple_of(index * plane_rows, plane_rows), plane_rows)

    def piece(index):
        return pl.ds(pl.multiple_of(index * chunk, chunk), chunk)

    loads = [
        pltpu.make_async_copy(k_in, kv_stage.at[0], load_sem.at[0]),
        pltpu.make_async_copy(v_in, kv_stage.at[1], load_sem.at[0]),
        pltpu.make_async_copy(q_in, q_stage, load_sem.at[1]),
    ]
    own = [
        pltpu.make_async_copy(k_in.at[:, cols(me, HEAD_DIM)], kv_all.at[0, position(me)], kv_recv),
        pltpu.make_async_copy(v_in.at[:, cols(me, HEAD_DIM)], kv_all.at[1, position(me)], kv_recv),
        pltpu.make_async_copy(q_in.at[:, cols(me, width)], q_all.at[block(me)], q_recv.at[near]),
    ]
    for copy in loads + own:
        copy.start()

    barrier = pltpu.get_barrier_semaphore()
    for d in range(1, members):
        pl.semaphore_signal(
            barrier, inc=1, device_id=member((me + d) % members), device_id_type=MESH
        )

    @pl.when(has_down)
    def _():
        for g in range(members):
            pl.semaphore_signal(barrier, inc=1, device_id=other_plane(-1, g), device_id_type=MESH)

    above = jnp.minimum(planes - 1 - plane, 1)
    pl.semaphore_wait(barrier, members - 1 + above * members)

    def kv_copy(src, dst, to):
        return pltpu.make_async_remote_copy(
            src_ref=kv_stage.at[:, :, cols(dst, HEAD_DIM)],
            dst_ref=kv_all.at[:, position(src)],
            send_sem=kv_send,
            recv_sem=kv_recv,
            device_id=member(to),
            device_id_type=MESH,
        )

    def q_copy(src, dst, to):
        return pltpu.make_async_remote_copy(
            src_ref=q_stage.at[:, cols(dst, width)],
            dst_ref=q_all.at[block(src)],
            send_sem=q_send,
            recv_sem=q_recv.at[src // per_chunk],
            device_id=member(to),
            device_id_type=MESH,
        )

    def up_copy(index):
        return pltpu.make_async_remote_copy(
            src_ref=kv_all.at[:, piece(index)],
            dst_ref=kv_all.at[:, piece(index)],
            send_sem=up_send.at[index],
            recv_sem=up_recv.at[index],
            device_id=other_plane(1),
            device_id_type=MESH,
        )

    def rise_copy(dst):
        return pltpu.make_async_remote_copy(
            src_ref=kv_stage.at[:, :, cols(dst, HEAD_DIM)],
            dst_ref=kv_all.at[:, position(me)],
            send_sem=rise_send,
            recv_sem=up_recv.at[plane * chunks + near],
            device_id=other_plane(1, dst),
            device_id_type=MESH,
        )

    def out_copy(src, dst, to):
        return pltpu.make_async_remote_copy(
            src_ref=result.at[block(dst)],
            dst_ref=out_ref.at[:, cols(src, width)],
            send_sem=out_send,
            recv_sem=out_recv,
            device_id=member(to),
            device_id_type=MESH,
        )

    base = me - core * heads

    def peer(mask):
        return flip(mask, base)

    def reach(mask):
        g = mask // heads
        return (mask % heads > 0) + 2 * (g // (2 if turns else 1) > 0)

    core_of = {m: (m // heads) % 2 if turns else 0 for m in range(members)}
    far_first = sorted(range(members), key=lambda m: (core_of[m], -reach(m), m))
    near_first = sorted(range(members), key=lambda m: (core_of[m], reach(m), m))

    def start_all(copy_of, order):
        for to in map(peer, order):

            @pl.when(to != me)
            def _(to=to):
                copy_of(me, to, to).start()

    def wait_all(ref, sem):
        pltpu.make_async_copy(ref, ref, sem).wait()

    wait_all(kv_stage, load_sem.at[0])
    wait_all(q_stage, load_sem.at[1])

    for side in range(1 + max(core_of.values())):
        @pl.when(has_up)
        def _(side=side):
            for mask in far_first:
                if core_of[mask] == side:
                    rise_copy(peer(mask)).start()

        start_all(kv_copy, [m for m in far_first if core_of[m] == side])

        start_all(q_copy, [m for m in near_first if core_of[m] == side])

    def receive(index):
        wait_all(kv_all.at[:, piece(index)], up_recv.at[index])

        @pl.when(has_up)
        def _():
            up_copy(index).start()

    def nearest(c):
        return (near + c) % chunks

    def chunk_of(step, c):
        return (plane - step) * chunks + nearest(c)

    ahead = jnp.minimum(plane, 1)
    if turns:
        ahead = plane
    ahead = jnp.where(has_up, ahead, 0)

    def forward(step, carry):
        for c in range(chunks):
            receive(chunk_of(step, c))
        return carry

    relays = has_up & has_down
    leads = relays & (core == 0) & turns
    trails = relays & (core == 1) & turns

    def lead_sent(first, last):
        for c in range(first, last):
            up_copy(chunk_of(plane, c)).wait_send()

    def pass_turn():
        sibling = {"head": head, "seq": seq + 1}
        pl.semaphore_signal(go_sem, inc=1, device_id=sibling, device_id_type=MESH)

    def take_turn():
        pl.semaphore_wait(go_sem, 1)

    scale = math.log2(math.e) / math.sqrt(HEAD_DIM)
    sub = chunk // 2 if chunk >= 2 * HEAD_DIM else chunk
    per_sub = sub // rows

    def attend(at_keys, row0, size, first=False):
        keys = kv_all[0, at_keys, :]
        count = keys.shape[0]
        ones = jnp.ones((count, HEAD_DIM), jnp.bfloat16)
        values = jnp.concatenate([kv_all[1, at_keys, :], ones], axis=1)
        for j in range(group):
            q = q_all[pl.ds(pl.multiple_of(row0, size), size), j * HEAD_DIM:(j + 1) * HEAD_DIM]
            at = pl.ds(pl.multiple_of(j * plane_rows + row0, size), size)
            score = lax.dot_general(
                q, keys, (((1,), (1,)), ((), ())), preferred_element_type=jnp.float32
            )
            if first:
                row = lax.broadcasted_iota(jnp.int32, score.shape, 0) + (count - size)
                col = lax.broadcasted_iota(jnp.int32, score.shape, 1)
                score = jnp.where(col <= row, score, NEG)
            top = jnp.broadcast_to(jnp.max(score, axis=1, keepdims=True), (size, HEAD_DIM))
            if not first:
                before = largest[at, :]
                top = jnp.maximum(before, top)
            spread = jnp.concatenate([top] * (count // HEAD_DIM), axis=1)
            weight = jnp.exp2((score - spread) * scale).astype(jnp.bfloat16)
            product = jnp.dot(weight, values, preferred_element_type=jnp.float32)
            if first:
                summed[at, :] = product
            else:
                shrink = jnp.exp2((before - top) * scale)
                summed[at, :] = summed[at, :] * jnp.concatenate([shrink, shrink], axis=1) + product
            largest[at, :] = top

    def own_tile(shift):
        for r in range(chunks):

            @pl.when(nearest(shift) == r)
            def _(r=r):
                at_keys = pl.ds(pl.multiple_of(plane * plane_rows, plane_rows), (r + 1) * chunk)
                attend(at_keys, r * chunk, chunk, first=True)

    if turns:

        @pl.when(leads)
        def _():
            lax.fori_loop(1, plane + 1, forward, 0)

            @pl.when(plane == 1)
            def _():
                lead_sent(0, chunks)
                pass_turn()

        @pl.when(trails)
        def _():
            @pl.when(plane == 1)
            def _():
                take_turn()
                forward(1, 0)

            @pl.when(plane > 1)
            def _():
                receive(chunk_of(1, 0))

    else:
        lax.fori_loop(1, ahead + 1, forward, 0)

    wait_all(kv_all.at[:, plane_of(plane)], kv_recv)
    wait_all(q_all.at[piece(near)], q_recv.at[near])
    own_tile(0)

    if turns:

        @pl.when(trails & (plane > 1))
        def _():
            take_turn()
            for c in range(1, chunks):
                receive(chunk_of(1, c))
            lax.fori_loop(2, plane, forward, 0)
            for c in range(chunks - 1):
                receive(chunk_of(plane, c))

    for shift in range(1, chunks):
        wait_all(q_all.at[piece(nearest(shift))], q_recv.at[nearest(shift)])
        own_tile(shift)

    if turns:

        @pl.when(leads & (plane > 1))
        def _():
            lead_sent(0, 1)
            pass_turn()

        @pl.when(trails & (plane > 1))
        def _():
            receive(chunk_of(plane, chunks - 1))

    def arrive(step, c):
        @pl.when(step > ahead)
        def _():
            receive(chunk_of(step, c))

    def whole_step(step, carry):
        for c in range(chunks):
            arrive(step, c)
        for row0 in range(0, plane_rows, chunk):
            attend(plane_of(plane - step), row0, chunk)
        return carry

    lax.fori_loop(1, plane, whole_step, 0)

    final = piece(chunk_of(plane, chunks - 1))

    @pl.when(has_down)
    def _():
        for c in range(chunks - 1):
            arrive(plane, c)
            for r in range(chunks):
                attend(piece(chunk_of(plane, c)), r * chunk, chunk)
        arrive(plane, chunks - 1)

    def finish(g):
        for j in range(group):
            at = pl.ds(pl.multiple_of(j * plane_rows + g * rows, rows), rows)
            result[block(g), j * HEAD_DIM:(j + 1) * HEAD_DIM] = (
                summed[at, :HEAD_DIM] / summed[at, HEAD_DIM:]
            ).astype(jnp.bfloat16)

    def close(attending):
        for shift in reversed(range(chunks)):
            size = chunk if shift else chunk
            for s in range(0, chunk, size):
                row0 = nearest(shift) * chunk + s
                if attending:
                    attend(final, row0, size)
                for i in range(size // rows):
                    to = row0 // rows + (me + 1 + i) % (size // rows)
                    finish(to)
                    if shift:
                        out_copy(me, to, to).start()
                        continue

                    @pl.when(to != me)
                    def _(to=to):
                        out_copy(me, to, to).start()

    @pl.when(has_down)
    def _():
        close(True)

    @pl.when(plane == 0)
    def _():
        close(False)

    pltpu.make_async_copy(result.at[block(me)], out_ref.at[:, cols(me, width)], out_recv).start()

    others = (members - 1) * HEAD_DIM
    kv_sent = kv_stage.at[:, :, :others]
    q_sent = q_stage.at[:, :group * others]
    wait_all(kv_sent, kv_send)
    wait_all(q_sent, q_send)

    @pl.when(has_up)
    def _():
        def sent(index, carry):
            @pl.when((index != chunk_of(plane, 0)) | jnp.logical_not(leads & (plane > 1)))
            def _():
                up_copy(index).wait_send()

            return carry

        done = jnp.where(leads & (plane == 1), chunks, 0) if turns else 0
        lax.fori_loop(done, plane * chunks, sent, 0)
        wait_all(kv_stage, rise_send)

    wait_all(result.at[:(members - 1) * rows], out_send)
    wait_all(out_ref, out_recv)


def solution(mesh):
    heads, seqs = mesh.shape["head"], mesh.shape["seq"]

    def on_device(queries, keys, values):
        rows = queries.shape[0]
        members = keys.shape[1] // HEAD_DIM
        inner = members // heads
        planes = seqs // inner
        group = queries.shape[1] // keys.shape[1]
        plane_rows = members * rows
        chunk = math.gcd(plane_rows, TILE)
        total = planes * plane_rows
        chunks = plane_rows // chunk
        relayed = max(planes - 2, 1) * chunks
        raised = max(planes - 1, 1) * chunks
        dma = pltpu.SemaphoreType.DMA
        cfg = (heads, planes, inner, group, rows, chunk)
        return pl.pallas_call(
            functools.partial(kernel, cfg),
            out_shape=pltpu.VMEM(queries.shape, jnp.bfloat16),
            in_specs=[pl.BlockSpec(memory_space=pl.ANY)] * 3,
            out_specs=pl.BlockSpec(memory_space=pltpu.VMEM),
            scratch_shapes=[
                pltpu.VMEM(queries.shape, jnp.bfloat16),
                pltpu.VMEM((2,) + keys.shape, jnp.bfloat16),
                pltpu.VMEM((plane_rows, group * HEAD_DIM), jnp.bfloat16),
                pltpu.VMEM((2, total, HEAD_DIM), jnp.bfloat16),
                pltpu.VMEM((group * plane_rows, HEAD_DIM), jnp.float32),
                pltpu.VMEM((group * plane_rows, 2 * HEAD_DIM), jnp.float32),
                pltpu.VMEM((plane_rows, group * HEAD_DIM), jnp.bfloat16),
                dma((2,)),
                pltpu.SemaphoreType.REGULAR,
                dma(()),
                dma(()),
                dma(()),
                dma((chunks,)),
                dma(()),
                dma((relayed,)),
                dma((raised,)),
                dma(()),
                dma(()),
            ],
            compiler_params=pltpu.CompilerParams(collective_id=0, has_side_effects=True),
        )(queries, keys, values)

    spec = P(("seq", "head"), None)
    return jax.shard_map(
        on_device, mesh=mesh, in_specs=(spec, spec, spec), out_specs=spec, check_vma=False
    )
```
